32 devices in a mesh: section: 4 (over y, core), tensor: 2 (over x), dp: 4 (over z).
Axes of the slice: x: 2, y: 2, z: 4, core: 2. Of those that a mesh axis runs over, the one named last changes fastest.
Arguments:
- acts: bfloat16 [4, 8, 256, 2048], P('section', 'dp', 'tensor'), parts along dimension 1, may hold values from -6 to 6
- fresh: bfloat16 [8, 256, 2048], P('dp', 'tensor'), parts along dimension 0, may hold values from -6 to 6
- order: int32 [4, 2], P('section'), may hold values from 0 to 1
- ln_gain: float32 [4, 2048], P('section'), may hold values from 0.1 to 1.9
- ln_bias: float32 [4, 2048], P('section'), may hold values from -3 to 3
- wqkv: bfloat16 [4, 2048, 6144], P('section', None, 'tensor'), may hold values from -4 to 4
- wo: bfloat16 [4, 2048, 2048], P('section', 'tensor'), may hold values from -0.125 to 0.125
Outputs:
- section_out: bfloat16 [8, 4, 256, 2048], P('dp', 'section', 'tensor'), parts along dimension 0
- held: bfloat16 [4, 8, 256, 2048], P('section', 'dp', 'tensor'), parts along dimension 1
The draws below stay inside these ranges and needn't reach their ends.
There are 4 independent parts, one for each index of `dp`. The reference program is written for one: setup_inputs(seed, part) draws one part's arguments, and reference() takes and returns one part's arrays. A program takes and returns all parts, laid end to end along the dimension named above; an argument that names none is the same for every part. Nothing has to cross between parts.
All inputs are finite; a program needn't handle non-finite values.
Results may differ from the reference program's by a relative error of at most 0.017.
Values may be sent and summed in bfloat16 or wider, within the bound.
A program may use at most 64 MiB of HBM per device.

```python
import jax
import jax.numpy as jnp
from jax import lax

D = 2048
HEADS = 16
HD = 128
SEQ = 256
SLOTS = 2
TICKS = 2
SECTIONS = 4
N_TENSOR = 2


def draw_wqkv(key, part):
    first = jax.random.fold_in(jax.random.fold_in(key, 11), 0)
    base = jnp.clip(jax.random.normal(first, (SECTIONS, D, HEADS, 3, HD), jnp.float32), -6.0, 6.0) * D ** (-0.5)
    return base.reshape(SECTIONS, D, HEADS * 3 * HD).astype(jnp.bfloat16)


def with_ends(values, own_key, smallest, largest):
    longest = values.shape.index(max(values.shape))
    spots = []
    for shift in (0, 1):
        where = [jax.random.randint(jax.random.fold_in(own_key, axis), (), 0, length) for axis, length in enumerate(values.shape)]
        where[longest] = (where[longest] + shift) % values.shape[longest]
        spots.append(tuple(where))
    return values.at[spots[0]].set(smallest).at[spots[1]].set(largest)


def level_of(rng, shape, cuts, low, high):
    loudness = 1.0
    for axis_at, blocks in cuts:
        steps = jax.random.uniform(jax.random.fold_in(jax.random.fold_in(rng, 6), axis_at), (blocks,), jnp.float32, low / len(cuts), high / len(cuts))
        loudness = loudness * jnp.repeat(jnp.exp(steps), shape[axis_at] // blocks).reshape((-1,) + (1,) * (len(shape) - 1 - axis_at))
    return loudness


def normal_values(rng, shape, scale, limit, cuts=(), kind=jnp.bfloat16):
    entries = jax.random.normal(rng, shape, jnp.float32) * scale
    if len(cuts) > 0:
        entries = level_of(rng, shape, cuts, -0.22, 0.18) * entries
    return jnp.clip(entries, min=-limit, max=limit).astype(kind)


def setup_inputs(seed: int = 0, part: int = 0) -> dict:
    key_list = jax.random.split(jax.random.key(seed), 8)
    own_keys = jax.random.split(jax.random.fold_in(key_list[7], part), 8)
    acts = normal_values(own_keys[0], (SECTIONS, SLOTS, SEQ, D), 1.0, 6.0, ((0, 4), (2, 2)))
    fresh = normal_values(own_keys[1], (TICKS, SEQ, D), 1.0, 6.0, ((1, 2),))
    order = with_ends(jax.random.randint(key_list[2], (SECTIONS, TICKS), 0, SLOTS), jax.random.fold_in(key_list[2], 1), 0, SLOTS - 1).astype(jnp.int32)
    ln_gain = jnp.clip(1.0 + 0.18 * jax.random.normal(key_list[3], (SECTIONS, D), jnp.float32), 0.1, 1.9)
    ln_bias = normal_values(key_list[4], (SECTIONS, D), 0.5, 3.0, ((0, 4),), jnp.float32)
    wqkv = draw_wqkv(jax.random.fold_in(key_list[7], 71), part)
    wo = normal_values(key_list[6], (SECTIONS, HEADS * HD, D), (HEADS * HD) ** -0.5, 0.125, ((0, 4), (1, 2)))
    return {"acts": acts, "fresh": fresh, "order": order, "ln_gain": ln_gain, "ln_bias": ln_bias, "wqkv": wqkv, "wo": wo}


def normed(rows, gain, bias):
    values = rows.astype(jnp.float32)
    centred = values - lax.optimization_barrier(jnp.mean(values, axis=-1, keepdims=True))
    spread = lax.optimization_barrier(jnp.mean(centred * centred, axis=-1, keepdims=True))
    return (centred * lax.rsqrt(spread + 1e-06) * gain + bias).astype(jnp.bfloat16)

def layer(inputs):
    rows, gain, bias, w_in, w_out = inputs
    normal_rows = normed(rows, gain, bias)
    qkv = jnp.dot(normal_rows, w_in, preferred_element_type=jnp.float32).astype(jnp.bfloat16)
    grid = qkv.reshape(SEQ, HEADS, 3, HD).astype(jnp.float32)
    scores = jnp.einsum('qhe,khe->hqk', grid[:, :, 0], grid[:, :, 1]) / jnp.sqrt(jnp.float32(HD))
    probs = jax.nn.softmax(scores, axis=-1).astype(jnp.bfloat16)
    attn = jnp.einsum('hqk,khe->qhe', probs.astype(jnp.float32), grid[:, :, 2]).astype(jnp.bfloat16)
    grouped = attn.reshape(SEQ, N_TENSOR, HEADS // N_TENSOR * HD).astype(jnp.float32)
    wo_grouped = w_out.reshape(N_TENSOR, HEADS // N_TENSOR * HD, D).astype(jnp.float32)
    partial_value = jnp.einsum('sgc,gcd->gsd', grouped, wo_grouped).astype(jnp.bfloat16)
    partial_value = lax.optimization_barrier(partial_value)
    total = lax.optimization_barrier(jnp.sum(partial_value.astype(jnp.float32), axis=0))
    return (rows.astype(jnp.float32) + total).astype(jnp.bfloat16)

def reference(acts, fresh, order, ln_gain, ln_bias, wqkv, wo):
    slots = acts
    outputs = []
    slot_ids = jnp.arange(SLOTS, dtype=jnp.int32)
    for tick in range(TICKS):
        chosen = order[:, tick].astype(jnp.int32)
        picked = jnp.take_along_axis(slots, chosen[:, None, None, None], axis=1)[:, 0]
        results = lax.map(layer, (picked, ln_gain, ln_bias, wqkv, wo))
        outputs.append(results)
        incoming = jnp.concatenate([fresh[tick][None], results[:-1]], axis=0)
        marks = (slot_ids[None, :] == chosen[:, None])[:, :, None, None]
        slots = jnp.where(marks, incoming[:, None], slots)
    return (jnp.stack(outputs, axis=0), slots)
```

```python
import functools
import math

import jax
import jax.numpy as jnp
from jax import lax
from jax.experimental import pallas as pl
from jax.experimental.pallas import tpu as pltpu
from jax.sharding import PartitionSpec as P

HD = 128
EPS = 1e-06
CHUNK = 512
TILE = 1024
NORM_ROWS = 16
PIECE = 32
MESH = pl.DeviceIdType.MESH


def fitting(most, size):
    return math.gcd(most, size)


def rs_spans(width):
    chunk = fitting(CHUNK, width)
    half = fitting(chunk // 2, width)
    sizes = [chunk] * (width // chunk - 1) + [half] * (chunk // half)
    return [(sum(sizes[:i]), size) for i, size in enumerate(sizes)]


def relay(
    acts, fresh, order_h, gain_h, bias_h, w_in, w_out, out, held,
    order, gain, bias, slots, fresh_v, wi, wo, xs, hs, acc, qkv, mixed, part, got, arr,
    small_sem, acts_sem, fresh_sem, wi_sem, wo_sem,
    ag_send, ag_recv, rs_send, rs_recv, hop_send, hop_recv, turn,
):
    ticks, rows, width = fresh.shape
    n_slots = acts.shape[1]
    peers = lax.axis_size("tensor")
    sections = lax.axis_size("section")
    me = lax.axis_index("tensor")
    sec = lax.axis_index("section")
    heads = wi.shape[1] // (3 * HD)
    chunk = fitting(CHUNK, width)
    n_chunks = width // chunk
    wi_tile = fitting(TILE, wi.shape[1])
    n_tiles = wi.shape[1] // wi_tile
    has_prev = sec > 0
    has_next = sec < sections - 1
    late = lax.rem(sec, 2) == 1
    early = jnp.logical_not(late)
    leads = early & has_next
    parts = rs_spans(width)
    n_parts = len(parts)

    def span(c):
        return pl.ds(c * chunk, chunk)

    def part_span(c):
        return pl.ds(*parts[c])

    barrier = pltpu.get_barrier_semaphore()
    for d in range(1, peers):
        pl.semaphore_signal(
            barrier, inc=1, device_id={"tensor": lax.rem(me + d, peers)}, device_id_type=MESH
        )

    @pl.when(has_prev)
    def _():
        pl.semaphore_signal(barrier, inc=1, device_id={"section": sec - 1}, device_id_type=MESH)

    @pl.when(has_next)
    def _():
        pl.semaphore_signal(barrier, inc=1, device_id={"section": sec + 1}, device_id_type=MESH)

    def acts_copy(c):
        return pltpu.make_async_copy(acts.at[0, :, :, span(c)], slots.at[:, :, span(c)], acts_sem.at[c])

    small = [
        pltpu.make_async_copy(src, dst, small_sem.at[i])
        for i, (src, dst) in enumerate([(order_h, order), (gain_h, gain), (bias_h, bias)])
    ]
    small[0].start()
    for c in range(n_chunks):
        acts_copy(c).start()
    small[1].start()
    small[2].start()

    def wi_copy(i):
        cols = pl.ds(i * wi_tile, wi_tile)
        return pltpu.make_async_copy(w_in.at[0, :, cols], wi.at[:, cols], wi_sem.at[i])

    load_wo = pltpu.make_async_copy(w_out.at[0], wo, wo_sem)
    load_fresh = pltpu.make_async_copy(fresh, fresh_v, fresh_sem)

    def ag_copy(t, d, c):
        return pltpu.make_async_remote_copy(
            src_ref=hs.at[t, 0, :, span(c)],
            dst_ref=hs.at[t, d, :, span(c)],
            send_sem=ag_send.at[t, d - 1],
            recv_sem=ag_recv.at[t, d - 1, c],
            device_id={"tensor": lax.rem(me + d, peers)},
            device_id_type=MESH,
        )

    def rs_copy(t, d, c):
        return pltpu.make_async_remote_copy(
            src_ref=part.at[t, d, :, part_span(c)],
            dst_ref=got.at[t, d - 1, :, part_span(c)],
            send_sem=rs_send.at[t, d - 1],
            recv_sem=rs_recv.at[t, d - 1, c],
            device_id={"tensor": lax.rem(me - d + peers, peers)},
            device_id_type=MESH,
        )

    def hop_copy(t, c):
        return pltpu.make_async_remote_copy(
            src_ref=out.at[t, 0, :, part_span(c)],
            dst_ref=arr.at[t, :, part_span(c)],
            send_sem=hop_send.at[t],
            recv_sem=hop_recv.at[t, c],
            device_id={"section": lax.rem(sec + 1, sections)},
            device_id_type=MESH,
        )

    def yield_turn(i, when):
        partner = sec + 1 - 2 * lax.rem(sec, 2)

        @pl.when(when)
        def _():
            pl.semaphore_signal(
                turn.at[i], inc=1, device_id={"section": partner}, device_id_type=MESH
            )

    def await_turn(i):
        with jax.named_scope(f"turn_{i}"):
            pl.semaphore_wait(turn.at[i], 1)

    def pieces(step):
        for i in range(rows // PIECE):
            step(pl.ds(i * PIECE, PIECE))

    def pick(t, values):
        chosen = order[0, t]
        x = values[0]
        for k in range(1, n_slots):
            x = jnp.where(chosen == k, values[k], x)
        return x

    def offer(t, c):
        def step(r):
            values = [slots[k, r, span(c)].astype(jnp.float32) for k in range(n_slots)]
            xs[t, r, span(c)] = pick(t, values).astype(jnp.bfloat16)

        pieces(step)

    def send_rows(t):
        for c in range(n_chunks):
            for d in range(1, peers):
                ag_copy(t, d, c).start()

    def norm(t):
        g = gain[0:1, :]
        b = bias[0:1, :]

        def one(i, carry):
            r = pl.ds(pl.multiple_of(i * NORM_ROWS, NORM_ROWS), NORM_ROWS)
            values = xs[t, r, :].astype(jnp.float32)
            centred = values - jnp.mean(values, axis=-1, keepdims=True)
            spread = jnp.mean(centred * centred, axis=-1, keepdims=True)
            hs[t, 0, r, :] = (centred * lax.rsqrt(spread + EPS) * g + b).astype(jnp.bfloat16)
            return carry

        lax.fori_loop(0, rows // NORM_ROWS, one, 0, unroll=4)

    def project(t):
        for i in range(n_tiles):
            if t == 0:
                wi_copy(i).wait()
            cols = pl.ds(i * wi_tile, wi_tile)
            y = jnp.dot(hs[t, 0], wi[:, cols], preferred_element_type=jnp.float32)
            qkv[0:rows, cols] = y.astype(jnp.bfloat16)

    def project_chunk(t, d, c):
        for i in range(n_tiles):
            cols = pl.ds(i * wi_tile, wi_tile)
            y = jnp.dot(
                hs[t, d, :, span(c)], wi[span(c), cols], preferred_element_type=jnp.float32
            )
            if c:
                y = acc[:, cols] + y
            if c + 1 < n_chunks:
                acc[:, cols] = y
            else:
                qkv[d * rows:(d + 1) * rows, cols] = y.astype(jnp.bfloat16)

    scale = math.log2(math.e) / math.sqrt(HD)

    def attend(t, d):
        r = slice(d * rows, (d + 1) * rows)
        for n in range(heads):
            base = n * 3 * HD
            q = qkv[r, base:base + HD]
            k = qkv[:, base + HD:base + 2 * HD]
            v = qkv[:, base + 2 * HD:base + 3 * HD]
            s = lax.dot_general(q, k, (((1,), (1,)), ((), ())), preferred_element_type=jnp.float32)
            e = jnp.exp2((s - jnp.max(s, axis=-1, keepdims=True)) * scale)
            total = jnp.sum(e, axis=-1, keepdims=True)
            y = jnp.dot(e.astype(jnp.bfloat16), v, preferred_element_type=jnp.float32)
            mixed[:, n * HD:(n + 1) * HD] = (y / total).astype(jnp.bfloat16)

        for c in range(n_parts):
            with jax.named_scope(f"wo_{t}_{d}_{c}"):
                y = jnp.dot(mixed[...], wo[:, part_span(c)], preferred_element_type=jnp.float32)
                part[t, d, :, part_span(c)] = y.astype(jnp.bfloat16)
                if d == 1 and c == 0:
                    @pl.when(late)
                    def _():
                        await_turn(1 + 2 * t)
                if d:
                    rs_copy(t, d, c).start()

    def finish(t):
        for c in range(n_parts):
            with jax.named_scope(f"rs_wait_{t}_{c}"):
                for d in range(1, peers):
                    rs_copy(t, d, c).wait_recv()
            if t == 0 and c == min(1, n_parts - 1):
                yield_turn(1, leads)

            def step(r):
                total = part[t, 0, r, part_span(c)].astype(jnp.float32)
                for d in range(1, peers):
                    total = total + got[t, d - 1, r, part_span(c)].astype(jnp.float32)
                x = xs[t, r, part_span(c)].astype(jnp.float32)
                out[t, 0, r, part_span(c)] = (x + total).astype(jnp.bfloat16)

            pieces(step)

            @pl.when(has_next)
            def _():
                hop_copy(t, c).start()

    def take(t):
        chosen = order[0, t]
        last = t + 1 == ticks

        def step(r, source, c):
            new = source[t, r, part_span(c)].astype(jnp.float32)
            values = [
                jnp.where(chosen == k, new, slots[k, r, part_span(c)].astype(jnp.float32))
                for k in range(n_slots)
            ]
            for k in range(n_slots):
                if last:
                    held[0, k, r, part_span(c)] = values[k].astype(jnp.bfloat16)
                else:
                    slots[k, r, part_span(c)] = values[k].astype(jnp.bfloat16)
            if not last:
                xs[t + 1, r, part_span(c)] = pick(t + 1, values).astype(jnp.bfloat16)

        for c in range(n_parts):
            @pl.when(has_prev)
            def _():
                with jax.named_scope(f"hop_wait_{t}_{c}"):
                    hop_copy(t, c).wait_recv()
                pieces(functools.partial(step, source=arr, c=c))

            @pl.when(jnp.logical_not(has_prev))
            def _():
                pieces(functools.partial(step, source=fresh_v, c=c))

    small[0].wait()
    for c in range(n_chunks):
        acts_copy(c).wait()
        if c + 1 == n_chunks:
            for i in range(n_tiles):
                wi_copy(i).start()
            load_wo.start()
            load_fresh.start()
        offer(0, c)
    small[1].wait()
    small[2].wait()
    with jax.named_scope("norm_first"):
        norm(0)
    with jax.named_scope("barrier"):
        pl.semaphore_wait(
            barrier, peers - 1 + has_prev.astype(jnp.int32) + has_next.astype(jnp.int32)
        )

    @pl.when(early)
    def _():
        send_rows(0)

    with jax.named_scope("project_first"):
        project(0)

    @pl.when(late)
    def _():
        await_turn(0)
        send_rows(0)

    for t in range(ticks):
        for d in range(1, peers):
            for c in range(n_chunks):
                with jax.named_scope(f"ag_wait_{t}_{c}"):
                    ag_copy(t, d, c).wait_recv()
                if d == 1 and c == min(1, n_chunks - 1):
                    yield_turn(3 * t, leads)
                    if t:
                        yield_turn(2, late)
                with jax.named_scope(f"pchunk_{t}_{c}"):
                    project_chunk(t, d, c)
        if t == 0:
            load_wo.wait()
        for d in [*range(1, peers), 0]:
            with jax.named_scope(f"attend_{t}_{d}"):
                attend(t, d)
        if t == 0:
            load_fresh.wait()
        if t + 1 == ticks:
            finish(t)
            take(t)
        else:
            @pl.when(early)
            def _():
                finish(t)

            take(t)
            with jax.named_scope(f"norm_{t}"):
                norm(t + 1)

            @pl.when(leads)
            def _():
                await_turn(2)

            send_rows(t + 1)

            @pl.when(late)
            def _():
                finish(t)

            with jax.named_scope(f"project_{t}"):
                project(t + 1)

    for t in range(ticks):
        for d in range(1, peers):
            for sem in (ag_send, rs_send):
                pltpu.make_async_copy(hs.at[t, 0], hs.at[t, 0], sem.at[t, d - 1]).wait()

        @pl.when(has_next)
        def _():
            pltpu.make_async_copy(hs.at[t, 0], hs.at[t, 0], hop_send.at[t]).wait()


def flush(out_v, held_v, out, held, sem):
    copies = [
        pltpu.make_async_copy(out_v, out, sem.at[0]),
        pltpu.make_async_copy(held_v, held, sem.at[1]),
    ]
    for copy in copies:
        copy.start()
    for copy in copies:
        copy.wait()


def pin(*xs):
    return [pltpu.with_memory_space_constraint(x, pltpu.HBM) for x in xs]


def body(acts, fresh, order, ln_gain, ln_bias, wqkv, wo):
    ticks, rows, width = fresh.shape
    n_slots = acts.shape[1]
    peers = lax.axis_size("tensor")
    seq = rows * peers
    n_chunks = width // fitting(CHUNK, width)
    n_parts = len(rs_spans(width))
    inner = wo.shape[1]
    wide = wqkv.shape[2]
    bf = jnp.bfloat16
    dma = pltpu.SemaphoreType.DMA
    anywhere = pl.BlockSpec(memory_space=pl.ANY)
    vmem = pl.BlockSpec(memory_space=pltpu.VMEM)
    out_shape = (ticks, 1, rows, width)
    held_shape = (1, n_slots, rows, width)
    results = pl.pallas_call(
        relay,
        out_shape=(pltpu.VMEM(out_shape, bf), pltpu.VMEM(held_shape, bf)),
        in_specs=[anywhere] * 7,
        out_specs=(vmem, vmem),
        scratch_shapes=[
            pltpu.SMEM(order.shape, jnp.int32),
            pltpu.VMEM(ln_gain.shape, jnp.float32),
            pltpu.VMEM(ln_bias.shape, jnp.float32),
            pltpu.VMEM((n_slots, rows, width), bf),
            pltpu.VMEM((ticks, rows, width), bf),
            pltpu.VMEM((width, wide), bf),
            pltpu.VMEM((inner, width), bf),
            pltpu.VMEM((ticks, rows, width), bf),
            pltpu.VMEM((ticks, peers, rows, width), bf),
            pltpu.VMEM((rows, wide), jnp.float32),
            pltpu.VMEM((seq, wide), bf),
            pltpu.VMEM((rows, inner), bf),
            pltpu.VMEM((ticks, peers, rows, width), bf),
            pltpu.VMEM((ticks, peers - 1, rows, width), bf),
            pltpu.VMEM((ticks, rows, width), bf),
            dma((3,)),
            dma((n_chunks,)),
            dma,
            dma((wide // fitting(TILE, wide),)),
            dma,
            dma((ticks, peers - 1)),
            dma((ticks, peers - 1, n_chunks)),
            dma((ticks, peers - 1)),
            dma((ticks, peers - 1, n_parts)),
            dma((ticks,)),
            dma((ticks, n_parts)),
            pltpu.SemaphoreType.REGULAR((4,)),
        ],
        compiler_params=pltpu.CompilerParams(
            collective_id=0, has_side_effects=True, vmem_limit_bytes=52 * 1024 * 1024
        ),
    )(*pin(acts, fresh, order, ln_gain, ln_bias, wqkv, wo))
    return pl.pallas_call(
        flush,
        out_shape=(jax.ShapeDtypeStruct(out_shape, bf), jax.ShapeDtypeStruct(held_shape, bf)),
        in_specs=[vmem, vmem],
        out_specs=(pl.BlockSpec(memory_space=pltpu.HBM), pl.BlockSpec(memory_space=pltpu.HBM)),
        scratch_shapes=[dma((2,))],
    )(*[pltpu.with_memory_space_constraint(x, pltpu.VMEM) for x in results])


def solution(mesh):
    return jax.shard_map(
        body,
        mesh=mesh,
        in_specs=(
            P("section", "dp", "tensor", None),
            P("dp", "tensor", None),
            P("section", None),
            P("section", None),
            P("section", None),
            P("section", None, "tensor"),
            P("section", "tensor", None),
        ),
        out_specs=(P("dp", "section", "tensor", None), P("section", "dp", "tensor", None)),
        check_vma=False,
    )
```

```python
import functools
import math

import jax
import jax.numpy as jnp
from jax import lax
from jax.experimental import pallas as pl
from jax.experimental.pallas import tpu as pltpu
from jax.sharding import PartitionSpec as P

HD = 128
EPS = 1e-06
CHUNK = 512
TILE = 1024
NORM_ROWS = 16
PIECE = 32
MESH = pl.DeviceIdType.MESH


def fitting(most, size):
    return math.gcd(most, size)


def spans(sizes):
    return [(sum(sizes[:i]), size) for i, size in enumerate(sizes)]


def ag_spans(width):
    chunk = fitting(CHUNK, width)
    half = chunk // 2
    if width < 2 * chunk:
        return spans([chunk])
    return spans([chunk] * (width // chunk - 2) + [half, chunk, half])


def rs_spans(width):
    chunk = fitting(CHUNK, width)
    half = chunk // 2
    return spans([chunk] * (width // chunk - 1) + [half, half])


def relay(
    acts, fresh, order_h, gain_h, bias_h, w_in, w_out, out, held,
    order, gain, bias, slots, fresh_v, wi, wo, xs, hs, acc, qkv, mixed, part, got, arr,
    small_sem, acts_sem, fresh_sem, wi_sem, wo_sem,
    ag_send, ag_recv, rs_send, rs_recv, hop_send, hop_recv, turn,
):
    ticks, rows, width = fresh.shape
    n_slots = acts.shape[1]
    peers = lax.axis_size("tensor")
    sections = lax.axis_size("section")
    me = lax.axis_index("tensor")
    sec = lax.axis_index("section")
    heads = wi.shape[1] // (3 * HD)
    wi_tile = fitting(TILE, wi.shape[1])
    n_tiles = wi.shape[1] // wi_tile
    has_prev = sec > 0
    has_next = sec < sections - 1
    late = lax.rem(sec, 2) == 1
    early = jnp.logical_not(late)
    leads = early & has_next
    chunks = ag_spans(width)
    n_chunks = len(chunks)
    n_lead = max(1, n_chunks - 2)
    lead_cols = sum(size for _, size in chunks[:n_lead])
    parts = rs_spans(width)
    n_parts = len(parts)

    def span(c):
        return pl.ds(*chunks[c])

    def part_span(c):
        return pl.ds(*parts[c])

    barrier = pltpu.get_barrier_semaphore()
    for d in range(1, peers):
        pl.semaphore_signal(
            barrier, inc=1, device_id={"tensor": lax.rem(me + d, peers)}, device_id_type=MESH
        )

    @pl.when(has_prev)
    def _():
        pl.semaphore_signal(barrier, inc=1, device_id={"section": sec - 1}, device_id_type=MESH)

    @pl.when(has_next)
    def _():
        pl.semaphore_signal(barrier, inc=1, device_id={"section": sec + 1}, device_id_type=MESH)

    def acts_copy(c):
        return pltpu.make_async_copy(acts.at[0, :, :, span(c)], slots.at[:, :, span(c)], acts_sem.at[c])

    small = [
        pltpu.make_async_copy(src, dst, small_sem.at[i])
        for i, (src, dst) in enumerate([(order_h, order), (gain_h, gain), (bias_h, bias)])
    ]
    small[0].start()
    for c in range(n_chunks):
        acts_copy(c).start()
    small[1].start()
    small[2].start()

    def wi_copy(i):
        cols = pl.ds(i * wi_tile, wi_tile)
        return pltpu.make_async_copy(w_in.at[0, :, cols], wi.at[:, cols], wi_sem.at[i])

    load_wo = pltpu.make_async_copy(w_out.at[0], wo, wo_sem)
    load_fresh = pltpu.make_async_copy(fresh, fresh_v, fresh_sem)

    def ag_copy(t, d, c):
        return pltpu.make_async_remote_copy(
            src_ref=hs.at[t, 0, :, span(c)],
            dst_ref=hs.at[t, d, :, span(c)],
            send_sem=ag_send.at[t, d - 1, int(c >= n_lead)],
            recv_sem=ag_recv.at[t, d - 1, c],
            device_id={"tensor": lax.rem(me + d, peers)},
            device_id_type=MESH,
        )

    def rs_copy(t, d, c):
        return pltpu.make_async_remote_copy(
            src_ref=part.at[t, d, :, part_span(c)],
            dst_ref=got.at[t, d - 1, :, part_span(c)],
            send_sem=rs_send.at[t, d - 1],
            recv_sem=rs_recv.at[t, d - 1, c],
            device_id={"tensor": lax.rem(me - d + peers, peers)},
            device_id_type=MESH,
        )

    def hop_copy(t, c):
        return pltpu.make_async_remote_copy(
            src_ref=out.at[t, 0, :, part_span(c)],
            dst_ref=arr.at[t, :, part_span(c)],
            send_sem=hop_send.at[t],
            recv_sem=hop_recv.at[t, c],
            device_id={"section": lax.rem(sec + 1, sections)},
            device_id_type=MESH,
        )

    def yield_turn(i, when):
        partner = sec + 1 - 2 * lax.rem(sec, 2)

        @pl.when(when)
        def _():
            pl.semaphore_signal(
                turn.at[i], inc=1, device_id={"section": partner}, device_id_type=MESH
            )

    def await_turn(i):
        with jax.named_scope(f"turn_{i}"):
            pl.semaphore_wait(turn.at[i], 1)

    def pieces(step):
        for i in range(rows // PIECE):
            step(pl.ds(i * PIECE, PIECE))

    def pick(t, values):
        chosen = order[0, t]
        x = values[0]
        for k in range(1, n_slots):
            x = jnp.where(chosen == k, values[k], x)
        return x

    def offer(t, c):
        def step(r):
            values = [slots[k, r, span(c)].astype(jnp.float32) for k in range(n_slots)]
            xs[t, r, span(c)] = pick(t, values).astype(jnp.bfloat16)

        pieces(step)

    def sent(t, d, tail):
        cols = pl.ds(lead_cols, width - lead_cols) if tail else pl.ds(0, lead_cols)
        rows_sent = hs.at[t, 0, :, cols]
        pltpu.make_async_copy(rows_sent, rows_sent, ag_send.at[t, d - 1, tail]).wait()

    def send_rows(t):
        for c in range(n_chunks):
            for d in range(1, peers):
                ag_copy(t, d, c).start()

    def norm(t):
        g = gain[0:1, :]
        b = bias[0:1, :]

        def one(i, carry):
            r = pl.ds(pl.multiple_of(i * NORM_ROWS, NORM_ROWS), NORM_ROWS)
            values = xs[t, r, :].astype(jnp.float32)
            centred = values - jnp.mean(values, axis=-1, keepdims=True)
            spread = jnp.mean(centred * centred, axis=-1, keepdims=True)
            hs[t, 0, r, :] = (centred * lax.rsqrt(spread + EPS) * g + b).astype(jnp.bfloat16)
            return carry

        lax.fori_loop(0, rows // NORM_ROWS, one, 0, unroll=4)

    def project(t):
        for i in range(n_tiles):
            if t == 0:
                wi_copy(i).wait()
            cols = pl.ds(i * wi_tile, wi_tile)
            y = jnp.dot(hs[t, 0], wi[:, cols], preferred_element_type=jnp.float32)
            qkv[0:rows, cols] = y.astype(jnp.bfloat16)

    def project_chunk(t, d, c):
        for i in range(n_tiles):
            cols = pl.ds(i * wi_tile, wi_tile)
            y = jnp.dot(
                hs[t, d, :, span(c)], wi[span(c), cols], preferred_element_type=jnp.float32
            )
            if c:
                y = acc[:, cols] + y
            if c + 1 < n_chunks:
                acc[:, cols] = y
            else:
                qkv[d * rows:(d + 1) * rows, cols] = y.astype(jnp.bfloat16)

    scale = math.log2(math.e) / math.sqrt(HD)

    def attend(t, d):
        r = slice(d * rows, (d + 1) * rows)
        for n in range(heads):
            base = n * 3 * HD
            q = qkv[r, base:base + HD]
            k = qkv[:, base + HD:base + 2 * HD]
            v = qkv[:, base + 2 * HD:base + 3 * HD]
            s = lax.dot_general(q, k, (((1,), (1,)), ((), ())), preferred_element_type=jnp.float32)
            e = jnp.exp2((s - jnp.max(s, axis=-1, keepdims=True)) * scale)
            total = jnp.sum(e, axis=-1, keepdims=True)
            y = jnp.dot(e.astype(jnp.bfloat16), v, preferred_element_type=jnp.float32)
            mixed[:, n * HD:(n + 1) * HD] = (y / total).astype(jnp.bfloat16)

        for c in range(n_parts):
            with jax.named_scope(f"wo_{t}_{d}_{c}"):
                y = jnp.dot(mixed[...], wo[:, part_span(c)], preferred_element_type=jnp.float32)
                part[t, d, :, part_span(c)] = y.astype(jnp.bfloat16)
                if d == 1 and c == 0:
                    @pl.when(late)
                    def _():
                        await_turn(1 + 2 * t)
                if d:
                    rs_copy(t, d, c).start()

    def finish(t, c):
        with jax.named_scope(f"rs_wait_{t}_{c}"):
            for d in range(1, peers):
                rs_copy(t, d, c).wait_recv()
        if t == 0 and c == min(1, n_parts - 1):
            yield_turn(1, leads)

        def step(r):
            total = part[t, 0, r, part_span(c)].astype(jnp.float32)
            for d in range(1, peers):
                total = total + got[t, d - 1, r, part_span(c)].astype(jnp.float32)
            x = xs[t, r, part_span(c)].astype(jnp.float32)
            out[t, 0, r, part_span(c)] = (x + total).astype(jnp.bfloat16)

        pieces(step)

        @pl.when(has_next)
        def _():
            hop_copy(t, c).start()

    def take(t, c):
        chosen = order[0, t]
        last = t + 1 == ticks

        def step(r, source):
            new = source[t, r, part_span(c)].astype(jnp.float32)
            values = [
                jnp.where(chosen == k, new, slots[k, r, part_span(c)].astype(jnp.float32))
                for k in range(n_slots)
            ]
            for k in range(n_slots):
                if last:
                    held[0, k, r, part_span(c)] = values[k].astype(jnp.bfloat16)
                else:
                    slots[k, r, part_span(c)] = values[k].astype(jnp.bfloat16)
            if not last:
                xs[t + 1, r, part_span(c)] = pick(t + 1, values).astype(jnp.bfloat16)

        @pl.when(has_prev)
        def _():
            with jax.named_scope(f"hop_wait_{t}_{c}"):
                hop_copy(t, c).wait_recv()
            pieces(functools.partial(step, source=arr))

        @pl.when(jnp.logical_not(has_prev))
        def _():
            pieces(functools.partial(step, source=fresh_v))

    small[0].wait()
    for c in range(n_chunks):
        acts_copy(c).wait()
        if c + 1 == n_chunks:
            for i in range(n_tiles):
                wi_copy(i).start()
            load_wo.start()
            load_fresh.start()
        offer(0, c)
    small[1].wait()
    small[2].wait()
    with jax.named_scope("norm_first"):
        norm(0)
    with jax.named_scope("barrier"):
        pl.semaphore_wait(
            barrier, peers - 1 + has_prev.astype(jnp.int32) + has_next.astype(jnp.int32)
        )

    @pl.when(early)
    def _():
        send_rows(0)

    with jax.named_scope("project_first"):
        project(0)

    @pl.when(late)
    def _():
        await_turn(0)
        send_rows(0)

    for t in range(ticks):
        if t:
            @pl.when(leads)
            def _():
                with jax.named_scope(f"lead_{t}"):
                    for d in range(1, peers):
                        sent(t, d, 0)

            yield_turn(3, leads)
        for d in range(1, peers):
            for c in range(n_chunks):
                with jax.named_scope(f"ag_wait_{t}_{c}"):
                    ag_copy(t, d, c).wait_recv()
                if t and d == 1 and c == min(1, n_chunks - 1):
                    yield_turn(2, late)
                with jax.named_scope(f"pchunk_{t}_{c}"):
                    project_chunk(t, d, c)
                if t == 0 and d == 1 and c == 0:
                    yield_turn(0, leads)
        if t == 0:
            load_wo.wait()
        for d in [*range(1, peers), 0]:
            with jax.named_scope(f"attend_{t}_{d}"):
                attend(t, d)
        if t == 0:
            load_fresh.wait()
        if t + 1 == ticks:
            for c in range(n_parts):
                finish(t, c)
            for c in range(n_parts):
                take(t, c)
        else:
            ahead = max(n_parts - 3, 0)

            @pl.when(early)
            def _():
                for c in range(n_parts):
                    finish(t, c)
                for c in range(n_parts):
                    take(t, c)

            @pl.when(late)
            def _():
                for c in range(n_parts):
                    take(t, c)
                    if 0 <= c - 2 < ahead:
                        finish(t, c - 2)

            with jax.named_scope(f"norm_{t}"):
                norm(t + 1)

            @pl.when(leads)
            def _():
                await_turn(2)

            send_rows(t + 1)

            @pl.when(late)
            def _():
                for c in range(ahead, n_parts):
                    finish(t, c)

            with jax.named_scope(f"project_{t}"):
                project(t + 1)

    for t in range(ticks):
        for d in range(1, peers):
            if t:
                @pl.when(jnp.logical_not(leads))
                def _():
                    sent(t, d, 0)
            else:
                sent(t, d, 0)
            if n_lead < n_chunks:
                sent(t, d, 1)
            pltpu.make_async_copy(hs.at[t, 0], hs.at[t, 0], rs_send.at[t, d - 1]).wait()

        @pl.when(has_next)
        def _():
            pltpu.make_async_copy(hs.at[t, 0], hs.at[t, 0], hop_send.at[t]).wait()


def flush(out_v, held_v, out, held, sem):
    copies = [
        pltpu.make_async_copy(out_v, out, sem.at[0]),
        pltpu.make_async_copy(held_v, held, sem.at[1]),
    ]
    for copy in copies:
        copy.start()
    for copy in copies:
        copy.wait()


def pin(*xs):
    return [pltpu.with_memory_space_constraint(x, pltpu.HBM) for x in xs]


def body(acts, fresh, order, ln_gain, ln_bias, wqkv, wo):
    ticks, rows, width = fresh.shape
    n_slots = acts.shape[1]
    peers = lax.axis_size("tensor")
    seq = rows * peers
    n_chunks = len(ag_spans(width))
    n_parts = len(rs_spans(width))
    inner = wo.shape[1]
    wide = wqkv.shape[2]
    bf = jnp.bfloat16
    dma = pltpu.SemaphoreType.DMA
    anywhere = pl.BlockSpec(memory_space=pl.ANY)
    vmem = pl.BlockSpec(memory_space=pltpu.VMEM)
    out_shape = (ticks, 1, rows, width)
    held_shape = (1, n_slots, rows, width)
    results = pl.pallas_call(
        relay,
        out_shape=(pltpu.VMEM(out_shape, bf), pltpu.VMEM(held_shape, bf)),
        in_specs=[anywhere] * 7,
        out_specs=(vmem, vmem),
        scratch_shapes=[
            pltpu.SMEM(order.shape, jnp.int32),
            pltpu.VMEM(ln_gain.shape, jnp.float32),
            pltpu.VMEM(ln_bias.shape, jnp.float32),
            pltpu.VMEM((n_slots, rows, width), bf),
            pltpu.VMEM((ticks, rows, width), bf),
            pltpu.VMEM((width, wide), bf),
            pltpu.VMEM((inner, width), bf),
            pltpu.VMEM((ticks, rows, width), bf),
            pltpu.VMEM((ticks, peers, rows, width), bf),
            pltpu.VMEM((rows, wide), jnp.float32),
            pltpu.VMEM((seq, wide), bf),
            pltpu.VMEM((rows, inner), bf),
            pltpu.VMEM((ticks, peers, rows, width), bf),
            pltpu.VMEM((ticks, peers - 1, rows, width), bf),
            pltpu.VMEM((ticks, rows, width), bf),
            dma((3,)),
            dma((n_chunks,)),
            dma,
            dma((wide // fitting(TILE, wide),)),
            dma,
            dma((ticks, peers - 1, 2)),
            dma((ticks, peers - 1, n_chunks)),
            dma((ticks, peers - 1)),
            dma((ticks, peers - 1, n_parts)),
            dma((ticks,)),
            dma((ticks, n_parts)),
            pltpu.SemaphoreType.REGULAR((4,)),
        ],
        compiler_params=pltpu.CompilerParams(
            collective_id=0, has_side_effects=True, vmem_limit_bytes=52 * 1024 * 1024
        ),
    )(*pin(acts, fresh, order, ln_gain, ln_bias, wqkv, wo))
    return pl.pallas_call(
        flush,
        out_shape=(jax.ShapeDtypeStruct(out_shape, bf), jax.ShapeDtypeStruct(held_shape, bf)),
        in_specs=[vmem, vmem],
        out_specs=(pl.BlockSpec(memory_space=pltpu.HBM), pl.BlockSpec(memory_space=pltpu.HBM)),
        scratch_shapes=[dma((2,))],
    )(*[pltpu.with_memory_space_constraint(x, pltpu.VMEM) for x in results])


def solution(mesh):
    return jax.shard_map(
        body,
        mesh=mesh,
        in_specs=(
            P("section", "dp", "tensor", None),
            P("dp", "tensor", None),
            P("section", None),
            P("section", None),
            P("section", None),
            P("section", None, "tensor"),
            P("section", "tensor", None),
        ),
        out_specs=(P("dp", "section", "tensor", None), P("section", "dp", "tensor", None)),
        check_vma=False,
    )
```

```python
import functools
import math

import jax
import jax.numpy as jnp
from jax import lax
from jax.experimental import pallas as pl
from jax.experimental.pallas import tpu as pltpu
from jax.sharding import PartitionSpec as P

HD = 128
EPS = 1e-06
CHUNK = 512
TILE = 1024
NORM_ROWS = 16
PIECE = 32
MESH = pl.DeviceIdType.MESH


def fitting(most, size):
    return math.gcd(most, size)


def spans(sizes):
    return [(sum(sizes[:i]), size) for i, size in enumerate(sizes)]


def ag_spans(width):
    chunk = fitting(CHUNK, width)
    half = chunk // 2
    if width < 2 * chunk:
        return spans([chunk])
    return spans([chunk + half] + [chunk] * (width // chunk - 2) + [half])


def rs_spans(width):
    chunk = fitting(CHUNK, width)
    tail = chunk // 4
    return spans([chunk] * (width // chunk - 1) + [chunk - tail, tail])


def relay(
    acts, fresh, order_h, gain_h, bias_h, w_in, w_out, out, held,
    order, affine, slots, fresh_v, wi, wo, xs, hs, acc, qkv, mixed, part, got, arr,
    small_sem, acts_sem, fresh_sem, wi_sem, wo_sem,
    ag_send, ag_recv, rs_send, rs_recv, hop_send, hop_recv, turn,
):
    ticks, rows, width = fresh.shape
    n_slots = acts.shape[1]
    peers = lax.axis_size("tensor")
    sections = lax.axis_size("section")
    me = lax.axis_index("tensor")
    sec = lax.axis_index("section")
    heads = wi.shape[1] // (3 * HD)
    wi_tile = fitting(TILE, wi.shape[1])
    n_tiles = wi.shape[1] // wi_tile
    has_prev = sec > 0
    has_next = sec < sections - 1
    late = lax.rem(sec, 2) == 1
    early = jnp.logical_not(late)
    leads = early & has_next
    chunks = ag_spans(width)
    n_chunks = len(chunks)
    halves = 2
    block = rows // halves
    parts = rs_spans(width)
    n_parts = len(parts)

    def span(c):
        return pl.ds(*chunks[c])

    def part_span(c):
        return pl.ds(*parts[c])

    barrier = pltpu.get_barrier_semaphore()
    for d in range(1, peers):
        pl.semaphore_signal(
            barrier, inc=1, device_id={"tensor": lax.rem(me + d, peers)}, device_id_type=MESH
        )

    @pl.when(has_prev)
    def _():
        pl.semaphore_signal(barrier, inc=1, device_id={"section": sec - 1}, device_id_type=MESH)

    @pl.when(has_next)
    def _():
        pl.semaphore_signal(barrier, inc=1, device_id={"section": sec + 1}, device_id_type=MESH)

    def row_block(i):
        return pl.ds(i * block, block)

    def acts_copy(i):
        return pltpu.make_async_copy(
            acts.at[0, :, row_block(i)], slots.at[:, row_block(i)], acts_sem.at[i]
        )

    load_order = pltpu.make_async_copy(order_h, order, small_sem.at[0])
    load_order.start()
    acts_copy(0).start()
    pltpu.make_async_copy(gain_h, affine.at[0:1], small_sem.at[1]).start()
    pltpu.make_async_copy(bias_h, affine.at[1:2], small_sem.at[1]).start()
    for i in range(1, halves):
        acts_copy(i).start()

    def wi_copy(i):
        cols = pl.ds(i * wi_tile, wi_tile)
        return pltpu.make_async_copy(w_in.at[0, :, cols], wi.at[:, cols], wi_sem.at[i])

    load_wo = pltpu.make_async_copy(w_out.at[0], wo, wo_sem)
    load_fresh = pltpu.make_async_copy(fresh, fresh_v, fresh_sem)

    def ag_copy(t, d, c, r=slice(None), tail=0):
        return pltpu.make_async_remote_copy(
            src_ref=hs.at[t, 0, r, span(c)],
            dst_ref=hs.at[t, d, r, span(c)],
            send_sem=ag_send.at[t, d - 1, tail],
            recv_sem=ag_recv.at[t, d - 1, c],
            device_id={"tensor": lax.rem(me + d, peers)},
            device_id_type=MESH,
        )

    def rs_copy(t, d, c):
        return pltpu.make_async_remote_copy(
            src_ref=part.at[t, d, :, part_span(c)],
            dst_ref=got.at[t, d - 1, :, part_span(c)],
            send_sem=rs_send.at[t, d - 1],
            recv_sem=rs_recv.at[t, d - 1, c],
            device_id={"tensor": lax.rem(me - d + peers, peers)},
            device_id_type=MESH,
        )

    def hop_copy(t, c):
        return pltpu.make_async_remote_copy(
            src_ref=out.at[t, 0, :, part_span(c)],
            dst_ref=arr.at[t, :, part_span(c)],
            send_sem=hop_send.at[t],
            recv_sem=hop_recv.at[t, c],
            device_id={"section": lax.rem(sec + 1, sections)},
            device_id_type=MESH,
        )

    def yield_turn(i, when):
        partner = sec + 1 - 2 * lax.rem(sec, 2)

        @pl.when(when)
        def _():
            pl.semaphore_signal(
                turn.at[0], inc=1, device_id={"section": partner}, device_id_type=MESH
            )

    def await_turn(i):
        with jax.named_scope(f"turn_{i}"):
            pl.semaphore_wait(turn.at[0], 1)

    def pieces(step):
        for i in range(rows // PIECE):
            step(pl.ds(i * PIECE, PIECE))

    def pick(t, values):
        chosen = order[0, t]
        x = values[0]
        for k in range(1, n_slots):
            x = jnp.where(chosen == k, values[k], x)
        return x

    def send_rows(t, i):
        r = row_block(i)
        for c in range(n_chunks):
            for d in range(1, peers):
                ag_copy(t, d, c, r, int(i + 1 == halves and c > 0)).start()

    def sent(t, d, tail):
        def drain(r, cols):
            copied = hs.at[t, 0, r, cols]
            pltpu.make_async_copy(copied, copied, ag_send.at[t, d - 1, tail]).wait()

        first = chunks[0][1]
        if tail:
            if first < width:
                drain(row_block(halves - 1), pl.ds(first, width - first))
        else:
            drain(pl.ds(0, block * (halves - 1)), pl.ds(0, width))
            drain(row_block(halves - 1), pl.ds(0, first))

    def norm(t, i):
        g = affine[0:1, :]
        b = affine[1:2, :]
        step = fitting(NORM_ROWS, block)

        def one(n, carry):
            r = pl.ds(pl.multiple_of(i * block + n * step, step), step)
            if t:
                values = xs[t, r, :].astype(jnp.float32)
            else:
                values = pick(t, [slots[k, r, :].astype(jnp.float32) for k in range(n_slots)])
                xs[t, r, :] = values.astype(jnp.bfloat16)
            centred = values - jnp.mean(values, axis=-1, keepdims=True)
            spread = jnp.mean(centred * centred, axis=-1, keepdims=True)
            hs[t, 0, r, :] = (centred * lax.rsqrt(spread + EPS) * g + b).astype(jnp.bfloat16)
            return carry

        lax.fori_loop(0, block // step, one, 0, unroll=block // step)

    def project(t):
        for i in range(n_tiles):
            if t == 0:
                wi_copy(i).wait()
            cols = pl.ds(i * wi_tile, wi_tile)
            y = jnp.dot(hs[t, 0], wi[:, cols], preferred_element_type=jnp.float32)
            qkv[0:rows, cols] = y.astype(jnp.bfloat16)

    def project_chunk(t, d, c):
        for i in range(n_tiles):
            cols = pl.ds(i * wi_tile, wi_tile)
            y = jnp.dot(
                hs[t, d, :, span(c)], wi[span(c), cols], preferred_element_type=jnp.float32
            )
            if c:
                y = acc[:, cols] + y
            if c + 1 < n_chunks:
                acc[:, cols] = y
            else:
                qkv[d * rows:(d + 1) * rows, cols] = y.astype(jnp.bfloat16)

    scale = math.log2(math.e) / math.sqrt(HD)

    def attend(t, d):
        r = slice(d * rows, (d + 1) * rows)
        for n in range(heads):
            base = n * 3 * HD
            q = qkv[r, base:base + HD]
            k = qkv[:, base + HD:base + 2 * HD]
            v = qkv[:, base + 2 * HD:base + 3 * HD]
            s = lax.dot_general(q, k, (((1,), (1,)), ((), ())), preferred_element_type=jnp.float32)
            e = jnp.exp2((s - jnp.max(s, axis=-1, keepdims=True)) * scale)
            total = jnp.sum(e, axis=-1, keepdims=True)
            y = jnp.dot(e.astype(jnp.bfloat16), v, preferred_element_type=jnp.float32)
            mixed[:, n * HD:(n + 1) * HD] = (y / total).astype(jnp.bfloat16)

        for c in range(n_parts):
            with jax.named_scope(f"wo_{t}_{d}_{c}"):
                y = jnp.dot(mixed[...], wo[:, part_span(c)], preferred_element_type=jnp.float32)
                part[t, d, :, part_span(c)] = y.astype(jnp.bfloat16)
                if d == 1 and c == 0:
                    @pl.when(late)
                    def _():
                        await_turn(1 + 2 * t)
                if d:
                    rs_copy(t, d, c).start()

    def finish(t, c):
        with jax.named_scope(f"rs_wait_{t}_{c}"):
            for d in range(1, peers):
                rs_copy(t, d, c).wait_recv()
        if t == 0 and c == min(1, n_parts - 1):
            yield_turn(1, leads)

        def step(r):
            total = part[t, 0, r, part_span(c)].astype(jnp.float32)
            for d in range(1, peers):
                total = total + got[t, d - 1, r, part_span(c)].astype(jnp.float32)
            x = xs[t, r, part_span(c)].astype(jnp.float32)
            out[t, 0, r, part_span(c)] = (x + total).astype(jnp.bfloat16)

        pieces(step)

        @pl.when(has_next)
        def _():
            hop_copy(t, c).start()

    def take(t, c):
        chosen = order[0, t]
        last = t + 1 == ticks

        def step(r, source):
            new = source[t, r, part_span(c)].astype(jnp.float32)
            values = [
                jnp.where(chosen == k, new, slots[k, r, part_span(c)].astype(jnp.float32))
                for k in range(n_slots)
            ]
            for k in range(n_slots):
                if last:
                    held[0, k, r, part_span(c)] = values[k].astype(jnp.bfloat16)
                else:
                    slots[k, r, part_span(c)] = values[k].astype(jnp.bfloat16)
            if not last:
                xs[t + 1, r, part_span(c)] = pick(t + 1, values).astype(jnp.bfloat16)

        @pl.when(has_prev)
        def _():
            with jax.named_scope(f"hop_wait_{t}_{c}"):
                hop_copy(t, c).wait_recv()
            pieces(functools.partial(step, source=arr))

        @pl.when(jnp.logical_not(has_prev))
        def _():
            pieces(functools.partial(step, source=fresh_v))

    def first_rows(i):
        with jax.named_scope(f"acts_wait_{i}"):
            acts_copy(i).wait()
            if i + 1 == halves:
                for n in range(n_tiles):
                    wi_copy(n).start()
                load_wo.start()
                load_fresh.start()
        with jax.named_scope(f"norm_first_{i}"):
            norm(0, i)

    with jax.named_scope("small_wait"):
        load_order.wait()
        pltpu.make_async_copy(affine, affine, small_sem.at[1]).wait()
    first_rows(0)
    with jax.named_scope("barrier"):
        pl.semaphore_wait(
            barrier, peers - 1 + has_prev.astype(jnp.int32) + has_next.astype(jnp.int32)
        )
    for i in range(halves):
        if i:
            first_rows(i)

        @pl.when(early)
        def _():
            send_rows(0, i)

    with jax.named_scope("project_first"):
        project(0)

    @pl.when(late)
    def _():
        await_turn(0)
        for i in range(halves):
            send_rows(0, i)

    yield_turn(0, leads)

    for t in range(ticks):
        if t:
            with jax.named_scope(f"lead_{t}"):
                for d in range(1, peers):
                    sent(t, d, 0)

            yield_turn(3, leads)
            yield_turn(2, late)
        for d in range(1, peers):
            for c in range(n_chunks):
                with jax.named_scope(f"ag_wait_{t}_{c}"):
                    ag_copy(t, d, c).wait_recv()
                with jax.named_scope(f"pchunk_{t}_{c}"):
                    project_chunk(t, d, c)
        if t == 0:
            load_wo.wait()
        for d in [*range(1, peers), 0]:
            with jax.named_scope(f"attend_{t}_{d}"):
                attend(t, d)
        if t == 0:
            load_fresh.wait()
        if t + 1 == ticks:
            for c in range(n_parts):
                finish(t, c)
            for c in range(n_parts):
                take(t, c)
        else:
            ahead = max(n_parts - 3, 0)

            @pl.when(early)
            def _():
                for c in range(n_parts):
                    finish(t, c)
                for c in range(n_parts):
                    take(t, c)

            @pl.when(late)
            def _():
                for c in range(n_parts):
                    take(t, c)
                    if 0 <= c - 2 < ahead:
                        finish(t, c - 2)

            for i in range(halves):
                with jax.named_scope(f"norm_{t}_{i}"):
                    norm(t + 1, i)
                if i == 0:
                    @pl.when(leads)
                    def _():
                        await_turn(2)

                send_rows(t + 1, i)

            @pl.when(late)
            def _():
                for c in range(ahead, n_parts):
                    finish(t, c)

            with jax.named_scope(f"project_{t}"):
                project(t + 1)

    for t in range(ticks):
        for d in range(1, peers):
            if t == 0:
                sent(t, d, 0)
            sent(t, d, 1)
            pltpu.make_async_copy(hs.at[t, 0], hs.at[t, 0], rs_send.at[t, d - 1]).wait()

        @pl.when(has_next)
        def _():
            pltpu.make_async_copy(hs.at[t, 0], hs.at[t, 0], hop_send.at[t]).wait()


def flush(out_v, held_v, out, held, sem):
    copies = [
        pltpu.make_async_copy(out_v, out, sem.at[0]),
        pltpu.make_async_copy(held_v, held, sem.at[1]),
    ]
    for copy in copies:
        copy.start()
    for copy in copies:
        copy.wait()


def pin(*xs):
    return [pltpu.with_memory_space_constraint(x, pltpu.HBM) for x in xs]


def body(acts, fresh, order, ln_gain, ln_bias, wqkv, wo):
    ticks, rows, width = fresh.shape
    n_slots = acts.shape[1]
    peers = lax.axis_size("tensor")
    seq = rows * peers
    n_chunks = len(ag_spans(width))
    n_parts = len(rs_spans(width))
    inner = wo.shape[1]
    wide = wqkv.shape[2]
    bf = jnp.bfloat16
    dma = pltpu.SemaphoreType.DMA
    anywhere = pl.BlockSpec(memory_space=pl.ANY)
    vmem = pl.BlockSpec(memory_space=pltpu.VMEM)
    out_shape = (ticks, 1, rows, width)
    held_shape = (1, n_slots, rows, width)
    results = pl.pallas_call(
        relay,
        out_shape=(pltpu.VMEM(out_shape, bf), pltpu.VMEM(held_shape, bf)),
        in_specs=[anywhere] * 7,
        out_specs=(vmem, vmem),
        scratch_shapes=[
            pltpu.SMEM(order.shape, jnp.int32),
            pltpu.VMEM((2, width), jnp.float32),
            pltpu.VMEM((n_slots, rows, width), bf),
            pltpu.VMEM((ticks, rows, width), bf),
            pltpu.VMEM((width, wide), bf),
            pltpu.VMEM((inner, width), bf),
            pltpu.VMEM((ticks, rows, width), bf),
            pltpu.VMEM((ticks, peers, rows, width), bf),
            pltpu.VMEM((rows, wide), jnp.float32),
            pltpu.VMEM((seq, wide), bf),
            pltpu.VMEM((rows, inner), bf),
            pltpu.VMEM((ticks, peers, rows, width), bf),
            pltpu.VMEM((ticks, peers - 1, rows, width), bf),
            pltpu.VMEM((ticks, rows, width), bf),
            dma((2,)),
            dma((2,)),
            dma,
            dma((wide // fitting(TILE, wide),)),
            dma,
            dma((ticks, peers - 1, 2)),
            dma((ticks, peers - 1, n_chunks)),
            dma((ticks, peers - 1)),
            dma((ticks, peers - 1, n_parts)),
            dma((ticks,)),
            dma((ticks, n_parts)),
            pltpu.SemaphoreType.REGULAR((1,)),
        ],
        compiler_params=pltpu.CompilerParams(
            collective_id=0, has_side_effects=True, vmem_limit_bytes=52 * 1024 * 1024
        ),
    )(*pin(acts, fresh, order, ln_gain, ln_bias, wqkv, wo))
    return pl.pallas_call(
        flush,
        out_shape=(jax.ShapeDtypeStruct(out_shape, bf), jax.ShapeDtypeStruct(held_shape, bf)),
        in_specs=[vmem, vmem],
        out_specs=(pl.BlockSpec(memory_space=pltpu.HBM), pl.BlockSpec(memory_space=pltpu.HBM)),
        scratch_shapes=[dma((2,))],
    )(*[pltpu.with_memory_space_constraint(x, pltpu.VMEM) for x in results])


def solution(mesh):
    return jax.shard_map(
        body,
        mesh=mesh,
        in_specs=(
            P("section", "dp", "tensor", None),
            P("dp", "tensor", None),
            P("section", None),
            P("section", None),
            P("section", None),
            P("section", None, "tensor"),
            P("section", "tensor", None),
        ),
        out_specs=(P("dp", "section", "tensor", None), P("section", "dp", "tensor", None)),
        check_vma=False,
    )
```

```python
import functools
import math

import jax
import jax.numpy as jnp
from jax import lax
from jax.experimental import pallas as pl
from jax.experimental.pallas import tpu as pltpu
from jax.sharding import PartitionSpec as P

HD = 128
EPS = 1e-06
CHUNK = 512
TILE = 1024
NORM_ROWS = 16
PIECE = 32
MESH = pl.DeviceIdType.MESH


def fitting(most, size):
    return math.gcd(most, size)


def spans(sizes):
    return [(sum(sizes[:i]), size) for i, size in enumerate(sizes)]


def ag_spans(width):
    chunk = fitting(CHUNK, width)
    half = chunk // 2
    if width < 2 * chunk:
        return spans([chunk])
    return spans([chunk + half] + [chunk] * (width // chunk - 2) + [half])


def rs_spans(width, last):
    chunk = fitting(CHUNK, width)
    tail = chunk // 4
    if last and width >= 2 * chunk:
        both = chunk - tail
        return spans([chunk] * (width // chunk - 2) + [2 * chunk - both, both])
    return spans([chunk] * (width // chunk - 1) + [chunk - tail, tail])


def relay(
    acts, fresh, order_h, gain_h, bias_h, w_in, w_out, out, held,
    order, affine, slots, fresh_v, wi, wo, xs, hs, acc, qkv, mixed, part, got, arr, duo,
    small_sem, acts_sem, fresh_sem, wi_sem, wo_sem,
    ag_send, ag_recv, rs_send, rs_recv, hop_send, hop_recv, duo_sem, turn,
):
    ticks, rows, width = fresh.shape
    n_slots = acts.shape[1]
    peers = lax.axis_size("tensor")
    sections = lax.axis_size("section")
    me = lax.axis_index("tensor")
    sec = lax.axis_index("section")
    heads = wi.shape[1] // (3 * HD)
    wi_tile = fitting(TILE, wi.shape[1])
    n_tiles = wi.shape[1] // wi_tile
    has_prev = sec > 0
    has_next = sec < sections - 1
    late = lax.rem(sec, 2) == 1
    early = jnp.logical_not(late)
    leads = early & has_next
    chunks = ag_spans(width)
    n_chunks = len(chunks)
    parts = [rs_spans(width, t + 1 == ticks) for t in range(ticks)]
    both = len(parts[-1]) - 1
    wo_tile = fitting(CHUNK, width)
    blocks = spans([rows // 4, rows - rows // 4])
    last_block = len(blocks) - 1

    def span(c):
        return pl.ds(*chunks[c])

    def part_span(t, c):
        return pl.ds(*parts[t][c])

    barrier = pltpu.get_barrier_semaphore()
    for d in range(1, peers):
        pl.semaphore_signal(
            barrier, inc=1, device_id={"tensor": lax.rem(me + d, peers)}, device_id_type=MESH
        )

    @pl.when(has_prev)
    def _():
        pl.semaphore_signal(barrier, inc=1, device_id={"section": sec - 1}, device_id_type=MESH)

    @pl.when(late)
    def _():
        for d in range(1, peers):
            pl.semaphore_signal(
                barrier, inc=1,
                device_id={"tensor": lax.rem(me + d, peers), "section": sec - 1},
                device_id_type=MESH,
            )

    @pl.when(has_next)
    def _():
        pl.semaphore_signal(barrier, inc=1, device_id={"section": sec + 1}, device_id_type=MESH)

    def row_block(i):
        return pl.ds(*blocks[i])

    def acts_copy(i):
        return pltpu.make_async_copy(
            acts.at[0, :, row_block(i)], slots.at[:, row_block(i)], acts_sem.at[i]
        )

    load_order = pltpu.make_async_copy(order_h, order, small_sem.at[0])
    load_order.start()
    acts_copy(0).start()
    pltpu.make_async_copy(gain_h, affine.at[0:1], small_sem.at[1]).start()
    pltpu.make_async_copy(bias_h, affine.at[1:2], small_sem.at[1]).start()
    for i in range(1, len(blocks)):
        acts_copy(i).start()

    def wi_copy(i):
        cols = pl.ds(i * wi_tile, wi_tile)
        return pltpu.make_async_copy(w_in.at[0, :, cols], wi.at[:, cols], wi_sem.at[i])

    load_wo = pltpu.make_async_copy(w_out.at[0], wo, wo_sem)
    load_fresh = pltpu.make_async_copy(fresh, fresh_v, fresh_sem)

    def ag_copy(t, d, c, r=slice(None), tail=0):
        return pltpu.make_async_remote_copy(
            src_ref=hs.at[t, 0, r, span(c)],
            dst_ref=hs.at[t, d, r, span(c)],
            send_sem=ag_send.at[t, d - 1, tail],
            recv_sem=ag_recv.at[t, d - 1, c],
            device_id={"tensor": lax.rem(me + d, peers)},
            device_id_type=MESH,
        )

    def rs_copy(t, d, c):
        return pltpu.make_async_remote_copy(
            src_ref=part.at[t, d, :, part_span(t, c)],
            dst_ref=got.at[t, d - 1, :, part_span(t, c)],
            send_sem=rs_send.at[t, d - 1],
            recv_sem=rs_recv.at[t, d - 1, c],
            device_id={"tensor": lax.rem(me - d + peers, peers)},
            device_id_type=MESH,
        )

    def hop_copy(t, c):
        return pltpu.make_async_remote_copy(
            src_ref=out.at[t, 0, :, part_span(t, c)],
            dst_ref=arr.at[t, :, part_span(t, c)],
            send_sem=hop_send.at[t],
            recv_sem=hop_recv.at[t, c],
            device_id={"section": lax.rem(sec + 1, sections)},
            device_id_type=MESH,
        )

    def shared(t):
        cols = part_span(t, both)
        sources = [xs.at[t, :, cols]] + [part.at[t, d, :, cols] for d in range(peers)]
        return [
            pltpu.make_async_remote_copy(
                src_ref=source,
                dst_ref=duo.at[i],
                send_sem=duo_sem.at[0],
                recv_sem=duo_sem.at[1],
                device_id={
                    "tensor": lax.rem(me - max(i - 1, 0) + peers, peers),
                    "section": lax.rem(sec + 1, sections),
                },
                device_id_type=MESH,
            )
            for i, source in enumerate(sources)
        ]

    def shared_wait(i):
        pltpu.make_async_copy(duo, duo, duo_sem.at[i]).wait()

    def yield_turn(i, when):
        partner = sec + 1 - 2 * lax.rem(sec, 2)

        @pl.when(when)
        def _():
            pl.semaphore_signal(
                turn.at[0], inc=1, device_id={"section": partner}, device_id_type=MESH
            )

    def await_turn(i):
        with jax.named_scope(f"turn_{i}"):
            pl.semaphore_wait(turn.at[0], 1)

    def pieces(step):
        for i in range(rows // PIECE):
            step(pl.ds(i * PIECE, PIECE))

    def pick(t, values):
        chosen = order[0, t]
        x = values[0]
        for k in range(1, n_slots):
            x = jnp.where(chosen == k, values[k], x)
        return x

    n_lead = max(1, n_chunks - 2)
    lead_cols = sum(size for _, size in chunks[:n_lead])

    def send_rows(t, i):
        for c in range(n_chunks):
            for d in range(1, peers):
                ag_copy(t, d, c, row_block(i), int(i == last_block and c >= n_lead)).start()

    def sent(t, d, tail):
        def drain(r, cols):
            copied = hs.at[t, 0, r, cols]
            pltpu.make_async_copy(copied, copied, ag_send.at[t, d - 1, tail]).wait()

        if tail:
            if lead_cols < width:
                drain(row_block(last_block), pl.ds(lead_cols, width - lead_cols))
        else:
            for i in range(last_block):
                drain(row_block(i), pl.ds(0, width))
            drain(row_block(last_block), pl.ds(0, lead_cols))

    def norm(t, i):
        g = affine[0:1, :]
        b = affine[1:2, :]
        start, size = blocks[i]
        step = fitting(NORM_ROWS, size)

        def one(n, carry):
            r = pl.ds(pl.multiple_of(start + n * step, step), step)
            if t:
                values = xs[t, r, :].astype(jnp.float32)
            else:
                values = pick(t, [slots[k, r, :].astype(jnp.float32) for k in range(n_slots)])
                xs[t, r, :] = values.astype(jnp.bfloat16)
            centred = values - jnp.mean(values, axis=-1, keepdims=True)
            spread = jnp.mean(centred * centred, axis=-1, keepdims=True)
            hs[t, 0, r, :] = (centred * lax.rsqrt(spread + EPS) * g + b).astype(jnp.bfloat16)
            return carry

        lax.fori_loop(0, size // step, one, 0, unroll=size // step)

    def project(t):
        for i in range(n_tiles):
            if t == 0:
                wi_copy(i).wait()
            cols = pl.ds(i * wi_tile, wi_tile)
            y = jnp.dot(hs[t, 0], wi[:, cols], preferred_element_type=jnp.float32)
            qkv[0:rows, cols] = y.astype(jnp.bfloat16)

    def project_chunk(t, d, c):
        for i in range(n_tiles):
            cols = pl.ds(i * wi_tile, wi_tile)
            y = jnp.dot(
                hs[t, d, :, span(c)], wi[span(c), cols], preferred_element_type=jnp.float32
            )
            if c:
                y = acc[:, cols] + y
            if c + 1 < n_chunks:
                acc[:, cols] = y
            else:
                qkv[d * rows:(d + 1) * rows, cols] = y.astype(jnp.bfloat16)

    scale = math.log2(math.e) / math.sqrt(HD)

    def attend(t, d):
        r = slice(d * rows, (d + 1) * rows)
        for n in range(heads):
            base = n * 3 * HD
            q = qkv[r, base:base + HD]
            k = qkv[:, base + HD:base + 2 * HD]
            v = qkv[:, base + 2 * HD:base + 3 * HD]
            s = lax.dot_general(q, k, (((1,), (1,)), ((), ())), preferred_element_type=jnp.float32)
            e = jnp.exp2((s - jnp.max(s, axis=-1, keepdims=True)) * scale)
            total = jnp.sum(e, axis=-1, keepdims=True)
            y = jnp.dot(e.astype(jnp.bfloat16), v, preferred_element_type=jnp.float32)
            mixed[:, n * HD:(n + 1) * HD] = (y / total).astype(jnp.bfloat16)

        ready = 0
        for j in range(width // wo_tile):
            cols = pl.ds(j * wo_tile, wo_tile)
            with jax.named_scope(f"wo_{t}_{d}_{j}"):
                y = jnp.dot(mixed[...], wo[:, cols], preferred_element_type=jnp.float32)
                part[t, d, :, cols] = y.astype(jnp.bfloat16)
                if d == 1 and j == 0:
                    @pl.when(late)
                    def _():
                        await_turn(1 + 2 * t)
                while d and ready < len(parts[t]) and sum(parts[t][ready]) <= (j + 1) * wo_tile:
                    rs_copy(t, d, ready).start()
                    ready += 1
        if t + 1 == ticks:
            @pl.when(leads)
            def _():
                copies = shared(t)
                for copy in [copies[1 + d]] if d else copies[:2]:
                    copy.start()

    def hops(t, c):
        return has_next & late if t + 1 == ticks and c == both else has_next

    def finish(t, c):
        with jax.named_scope(f"rs_wait_{t}_{c}"):
            for d in range(1, peers):
                rs_copy(t, d, c).wait_recv()
        if t == 0 and c == min(1, len(parts[t]) - 1):
            yield_turn(1, leads)

        def step(r):
            total = part[t, 0, r, part_span(t, c)].astype(jnp.float32)
            for d in range(1, peers):
                total = total + got[t, d - 1, r, part_span(t, c)].astype(jnp.float32)
            x = xs[t, r, part_span(t, c)].astype(jnp.float32)
            out[t, 0, r, part_span(t, c)] = (x + total).astype(jnp.bfloat16)

        pieces(step)

        @pl.when(hops(t, c))
        def _():
            hop_copy(t, c).start()

    def take(t, c):
        chosen = order[0, t]
        last = t + 1 == ticks

        def step(r, source):
            if source is duo:
                total = duo[1, r, :].astype(jnp.float32)
                for d in range(1, peers):
                    total = total + duo[1 + d, r, :].astype(jnp.float32)
                new = (duo[0, r, :].astype(jnp.float32) + total).astype(jnp.bfloat16)
                new = new.astype(jnp.float32)
            else:
                new = source[t, r, part_span(t, c)].astype(jnp.float32)
            values = [
                jnp.where(chosen == k, new, slots[k, r, part_span(t, c)].astype(jnp.float32))
                for k in range(n_slots)
            ]
            for k in range(n_slots):
                if last:
                    held[0, k, r, part_span(t, c)] = values[k].astype(jnp.bfloat16)
                else:
                    slots[k, r, part_span(t, c)] = values[k].astype(jnp.bfloat16)
            if not last:
                xs[t + 1, r, part_span(t, c)] = pick(t + 1, values).astype(jnp.bfloat16)

        if last and c == both:
            @pl.when(late)
            def _():
                with jax.named_scope("shared_wait"):
                    shared_wait(1)
                pieces(functools.partial(step, source=duo))

            by_hop = has_prev & early
        else:
            by_hop = has_prev

        @pl.when(by_hop)
        def _():
            with jax.named_scope(f"hop_wait_{t}_{c}"):
                hop_copy(t, c).wait_recv()
            pieces(functools.partial(step, source=arr))

        @pl.when(jnp.logical_not(has_prev))
        def _():
            pieces(functools.partial(step, source=fresh_v))

    def first_rows(i):
        with jax.named_scope(f"acts_wait_{i}"):
            acts_copy(i).wait()
            if i == last_block:
                for n in range(n_tiles):
                    wi_copy(n).start()
                load_wo.start()
                load_fresh.start()
        with jax.named_scope(f"norm_first_{i}"):
            norm(0, i)

    with jax.named_scope("small_wait"):
        load_order.wait()
        pltpu.make_async_copy(affine, affine, small_sem.at[1]).wait()
    first_rows(0)
    with jax.named_scope("barrier"):
        pl.semaphore_wait(
            barrier,
            (peers - 1) * (1 + leads.astype(jnp.int32))
            + has_prev.astype(jnp.int32) + has_next.astype(jnp.int32),
        )
    for i in range(len(blocks)):
        if i:
            first_rows(i)

        @pl.when(early)
        def _():
            send_rows(0, i)

    with jax.named_scope("project_first"):
        project(0)

    @pl.when(late)
    def _():
        await_turn(0)
        for i in range(len(blocks)):
            send_rows(0, i)

    yield_turn(0, leads)

    for t in range(ticks):
        if t:
            with jax.named_scope(f"lead_{t}"):
                for d in range(1, peers):
                    sent(t, d, 0)

            yield_turn(3, leads)
            yield_turn(2, late)
        for d in range(1, peers):
            for c in range(n_chunks):
                with jax.named_scope(f"ag_wait_{t}_{c}"):
                    ag_copy(t, d, c).wait_recv()
                with jax.named_scope(f"pchunk_{t}_{c}"):
                    project_chunk(t, d, c)
        if t == 0:
            load_wo.wait()
        for d in [*range(1, peers), 0]:
            with jax.named_scope(f"attend_{t}_{d}"):
                attend(t, d)
        if t == 0:
            load_fresh.wait()
        if t + 1 == ticks:
            for c in range(len(parts[t])):
                finish(t, c)
            for c in range(len(parts[t])):
                take(t, c)
        else:
            ahead = max(len(parts[t]) - 3, 0)

            @pl.when(early)
            def _():
                for c in range(len(parts[t])):
                    finish(t, c)
                for c in range(len(parts[t])):
                    take(t, c)

            @pl.when(late)
            def _():
                for c in range(len(parts[t])):
                    take(t, c)
                    if 0 <= c - 2 < ahead:
                        finish(t, c - 2)

            for i in range(len(blocks)):
                with jax.named_scope(f"norm_{t}_{i}"):
                    norm(t + 1, i)
                if i == 0:
                    @pl.when(leads)
                    def _():
                        await_turn(2)

                send_rows(t + 1, i)

            @pl.when(late)
            def _():
                for c in range(ahead, len(parts[t])):
                    finish(t, c)

            with jax.named_scope(f"project_{t}"):
                project(t + 1)

    for t in range(ticks):
        for d in range(1, peers):
            if t == 0:
                sent(t, d, 0)
            sent(t, d, 1)
            pltpu.make_async_copy(hs.at[t, 0], hs.at[t, 0], rs_send.at[t, d - 1]).wait()

        def hopped(cols):
            copied = hs.at[t, 0, :, cols]
            pltpu.make_async_copy(copied, copied, hop_send.at[t]).wait()

        if t + 1 < ticks:
            @pl.when(has_next)
            def _():
                hopped(pl.ds(0, width))
        else:
            @pl.when(has_next & late)
            def _():
                hopped(pl.ds(0, width))

            @pl.when(leads)
            def _():
                hopped(pl.ds(0, parts[t][both][0]))
                shared_wait(0)


def flush(out_v, held_v, out, held, sem):
    copies = [
        pltpu.make_async_copy(out_v, out, sem.at[0]),
        pltpu.make_async_copy(held_v, held, sem.at[1]),
    ]
    for copy in copies:
        copy.start()
    for copy in copies:
        copy.wait()


def pin(*xs):
    return [pltpu.with_memory_space_constraint(x, pltpu.HBM) for x in xs]


def body(acts, fresh, order, ln_gain, ln_bias, wqkv, wo):
    ticks, rows, width = fresh.shape
    n_slots = acts.shape[1]
    peers = lax.axis_size("tensor")
    seq = rows * peers
    n_chunks = len(ag_spans(width))
    n_parts = max(len(rs_spans(width, last)) for last in (False, True))
    inner = wo.shape[1]
    wide = wqkv.shape[2]
    bf = jnp.bfloat16
    dma = pltpu.SemaphoreType.DMA
    anywhere = pl.BlockSpec(memory_space=pl.ANY)
    vmem = pl.BlockSpec(memory_space=pltpu.VMEM)
    out_shape = (ticks, 1, rows, width)
    held_shape = (1, n_slots, rows, width)
    results = pl.pallas_call(
        relay,
        out_shape=(pltpu.VMEM(out_shape, bf), pltpu.VMEM(held_shape, bf)),
        in_specs=[anywhere] * 7,
        out_specs=(vmem, vmem),
        scratch_shapes=[
            pltpu.SMEM(order.shape, jnp.int32),
            pltpu.VMEM((2, width), jnp.float32),
            pltpu.VMEM((n_slots, rows, width), bf),
            pltpu.VMEM((ticks, rows, width), bf),
            pltpu.VMEM((width, wide), bf),
            pltpu.VMEM((inner, width), bf),
            pltpu.VMEM((ticks, rows, width), bf),
            pltpu.VMEM((ticks, peers, rows, width), bf),
            pltpu.VMEM((rows, wide), jnp.float32),
            pltpu.VMEM((seq, wide), bf),
            pltpu.VMEM((rows, inner), bf),
            pltpu.VMEM((ticks, peers, rows, width), bf),
            pltpu.VMEM((ticks, peers - 1, rows, width), bf),
            pltpu.VMEM((ticks, rows, width), bf),
            pltpu.VMEM((peers + 1, rows, rs_spans(width, True)[-1][1]), bf),
            dma((2,)),
            dma((2,)),
            dma,
            dma((wide // fitting(TILE, wide),)),
            dma,
            dma((ticks, peers - 1, 2)),
            dma((ticks, peers - 1, n_chunks)),
            dma((ticks, peers - 1)),
            dma((ticks, peers - 1, n_parts)),
            dma((ticks,)),
            dma((ticks, n_parts)),
            dma((2,)),
            pltpu.SemaphoreType.REGULAR((1,)),
        ],
        compiler_params=pltpu.CompilerParams(
            collective_id=0, has_side_effects=True, vmem_limit_bytes=52 * 1024 * 1024
        ),
    )(*pin(acts, fresh, order, ln_gain, ln_bias, wqkv, wo))
    return pl.pallas_call(
        flush,
        out_shape=(jax.ShapeDtypeStruct(out_shape, bf), jax.ShapeDtypeStruct(held_shape, bf)),
        in_specs=[vmem, vmem],
        out_specs=(pl.BlockSpec(memory_space=pltpu.HBM), pl.BlockSpec(memory_space=pltpu.HBM)),
        scratch_shapes=[dma((2,))],
    )(*[pltpu.with_memory_space_constraint(x, pltpu.VMEM) for x in results])


def solution(mesh):
    return jax.shard_map(
        body,
        mesh=mesh,
        in_specs=(
            P("section", "dp", "tensor", None),
            P("dp", "tensor", None),
            P("section", None),
            P("section", None),
            P("section", None),
            P("section", None, "tensor"),
            P("section", "tensor", None),
        ),
        out_specs=(P("dp", "section", "tensor", None), P("section", "dp", "tensor", None)),
        check_vma=False,
    )
```

```python
import functools
import math

import jax
import jax.numpy as jnp
from jax import lax
from jax.experimental import pallas as pl
from jax.experimental.pallas import tpu as pltpu
from jax.sharding import PartitionSpec as P

HD = 128
EPS = 1e-06
CHUNK = 512
TILE = 1024
NORM_ROWS = 16
PIECE = 32
MESH = pl.DeviceIdType.MESH


def fitting(most, size):
    return math.gcd(most, size)


def spans(sizes):
    return [(sum(sizes[:i]), size) for i, size in enumerate(sizes)]


def ag_spans(width):
    chunk = fitting(CHUNK, width)
    half = chunk // 2
    if width < 2 * chunk:
        return spans([chunk])
    return spans([chunk + half] + [chunk] * (width // chunk - 2) + [half])


def rs_spans(width):
    chunk = fitting(CHUNK, width)
    tail = chunk // 4
    if width < 2 * chunk:
        return spans([chunk - tail, tail])
    return spans([chunk] * (width // chunk - 2) + [chunk + tail, chunk - tail])


def relay(
    acts, fresh, order_h, gain_h, bias_h, w_in, w_out, out, held,
    order, affine, slots, fresh_v, wi, wo, xs, hs, acc, qkv, mixed, part, got, arr, duo, raw,
    small_sem, acts_sem, fresh_sem, wi_sem, wo_sem,
    ag_send, ag_recv, rs_send, rs_recv, hop_send, hop_recv, duo_sem, raw_sem, turn,
):
    ticks, rows, width = fresh.shape
    n_slots = acts.shape[1]
    peers = lax.axis_size("tensor")
    sections = lax.axis_size("section")
    me = lax.axis_index("tensor")
    sec = lax.axis_index("section")
    heads = wi.shape[1] // (3 * HD)
    wi_tile = fitting(TILE, wi.shape[1])
    n_tiles = wi.shape[1] // wi_tile
    has_prev = sec > 0
    has_next = sec < sections - 1
    late = lax.rem(sec, 2) == 1
    early = jnp.logical_not(late)
    leads = early & has_next
    chunks = ag_spans(width)
    n_chunks = len(chunks)
    parts = [rs_spans(width) for t in range(ticks)]
    both = len(parts[-1]) - 1
    wo_tile = fitting(CHUNK, width)
    blocks = spans([rows // 4, rows - rows // 4])
    last_block = len(blocks) - 1

    def span(c):
        return pl.ds(*chunks[c])

    def part_span(t, c):
        return pl.ds(*parts[t][c])

    barrier = pltpu.get_barrier_semaphore()
    for d in range(1, peers):
        pl.semaphore_signal(
            barrier, inc=1, device_id={"tensor": lax.rem(me + d, peers)}, device_id_type=MESH
        )

    @pl.when(has_prev)
    def _():
        pl.semaphore_signal(barrier, inc=1, device_id={"section": sec - 1}, device_id_type=MESH)

    @pl.when(late)
    def _():
        for d in range(1, peers):
            pl.semaphore_signal(
                barrier, inc=1,
                device_id={"tensor": lax.rem(me + d, peers), "section": sec - 1},
                device_id_type=MESH,
            )

    @pl.when(has_next)
    def _():
        pl.semaphore_signal(barrier, inc=1, device_id={"section": sec + 1}, device_id_type=MESH)

    def row_block(i):
        return pl.ds(*blocks[i])

    def acts_copy(i):
        return pltpu.make_async_copy(
            acts.at[0, :, row_block(i)], slots.at[:, row_block(i)], acts_sem.at[i]
        )

    load_order = pltpu.make_async_copy(order_h, order, small_sem.at[0])
    load_order.start()
    acts_copy(0).start()
    pltpu.make_async_copy(gain_h, affine.at[0:1], small_sem.at[1]).start()
    pltpu.make_async_copy(bias_h, affine.at[1:2], small_sem.at[1]).start()
    for i in range(1, len(blocks)):
        acts_copy(i).start()

    def wi_copy(i):
        cols = pl.ds(i * wi_tile, wi_tile)
        return pltpu.make_async_copy(w_in.at[0, :, cols], wi.at[:, cols], wi_sem.at[i])

    load_wo = pltpu.make_async_copy(w_out.at[0], wo, wo_sem)
    load_fresh = pltpu.make_async_copy(fresh, fresh_v, fresh_sem)

    def ag_copy(t, d, c, r=slice(None), tail=0):
        return pltpu.make_async_remote_copy(
            src_ref=hs.at[t, 0, r, span(c)],
            dst_ref=hs.at[t, d, r, span(c)],
            send_sem=ag_send.at[d - 1, tail],
            recv_sem=ag_recv.at[t, d - 1, c],
            device_id={"tensor": lax.rem(me + d, peers)},
            device_id_type=MESH,
        )

    def rs_copy(t, d, c):
        return pltpu.make_async_remote_copy(
            src_ref=part.at[t, d, :, part_span(t, c)],
            dst_ref=got.at[t, d - 1, :, part_span(t, c)],
            send_sem=rs_send.at[d - 1],
            recv_sem=rs_recv.at[t, d - 1, c],
            device_id={"tensor": lax.rem(me - d + peers, peers)},
            device_id_type=MESH,
        )

    def hop_copy(t, c):
        return pltpu.make_async_remote_copy(
            src_ref=out.at[t, 0, :, part_span(t, c)],
            dst_ref=arr.at[t, :, part_span(t, c)],
            send_sem=hop_send,
            recv_sem=hop_recv.at[t, c],
            device_id={"section": lax.rem(sec + 1, sections)},
            device_id_type=MESH,
        )

    def shared(t):
        cols = part_span(t, both)
        sources = [xs.at[t, :, cols]] + [part.at[t, d, :, cols] for d in range(peers)]
        return [
            pltpu.make_async_remote_copy(
                src_ref=source,
                dst_ref=duo.at[i],
                send_sem=duo_sem.at[0],
                recv_sem=duo_sem.at[1],
                device_id={
                    "tensor": lax.rem(me - max(i - 1, 0) + peers, peers),
                    "section": lax.rem(sec + 1, sections),
                },
                device_id_type=MESH,
            )
            for i, source in enumerate(sources)
        ]

    def shared_wait(i):
        pltpu.make_async_copy(duo, duo, duo_sem.at[i]).wait()

    def yield_turn(i, when):
        partner = sec + 1 - 2 * lax.rem(sec, 2)

        @pl.when(when)
        def _():
            pl.semaphore_signal(
                turn.at[0], inc=1, device_id={"section": partner}, device_id_type=MESH
            )

    def await_turn(i):
        with jax.named_scope(f"turn_{i}"):
            pl.semaphore_wait(turn.at[0], 1)

    def pieces(step):
        for i in range(rows // PIECE):
            step(pl.ds(i * PIECE, PIECE))

    def pick(t, values):
        chosen = order[0, t]
        x = values[0]
        for k in range(1, n_slots):
            x = jnp.where(chosen == k, values[k], x)
        return x

    n_lead = max(1, n_chunks - 2)
    lead_cols = sum(size for _, size in chunks[:n_lead])

    def raw_copy(d):
        return pltpu.make_async_remote_copy(
            src_ref=xs.at[0, row_block(0)],
            dst_ref=raw.at[d - 1],
            send_sem=ag_send.at[d - 1, 0],
            recv_sem=raw_sem.at[d - 1],
            device_id={"tensor": lax.rem(me + d, peers)},
            device_id_type=MESH,
        )

    def send_rows(t, i):
        if t == 0 and i == 0:
            for d in range(1, peers):
                raw_copy(d).start()
            return
        for c in range(n_chunks):
            for d in range(1, peers):
                ag_copy(t, d, c, row_block(i), int(i == last_block and c >= n_lead)).start()

    def sent(t, d, tail):
        def drain(r, cols):
            copied = hs.at[t, 0, r, cols]
            pltpu.make_async_copy(copied, copied, ag_send.at[d - 1, tail]).wait()

        if tail:
            if lead_cols < width:
                drain(row_block(last_block), pl.ds(lead_cols, width - lead_cols))
        else:
            for i in range(last_block):
                drain(row_block(i), pl.ds(0, width))
            drain(row_block(last_block), pl.ds(0, lead_cols))

    def gathered(t):
        for d in range(1, peers):
            if t == 0:
                sent(t, d, 0)
            sent(t, d, 1)

    def reduced(t):
        for d in range(1, peers):
            pltpu.make_async_copy(hs.at[t, 0], hs.at[t, 0], rs_send.at[d - 1]).wait()

    def hopped(t):
        def drain(cols):
            copied = hs.at[t, 0, :, cols]
            pltpu.make_async_copy(copied, copied, hop_send).wait()

        if t + 1 < ticks:
            @pl.when(has_next)
            def _():
                drain(pl.ds(0, width))
        else:
            @pl.when(has_next & late)
            def _():
                drain(pl.ds(0, width))

            @pl.when(leads)
            def _():
                drain(pl.ds(0, parts[t][both][0]))
                shared_wait(0)

    def offer(i):
        start, size = blocks[i]
        for n in range(size // PIECE):
            r = pl.ds(start + n * PIECE, PIECE)
            values = pick(0, [slots[k, r, :].astype(jnp.float32) for k in range(n_slots)])
            xs[0, r, :] = values.astype(jnp.bfloat16)

    def norm(t, i, source=None, d=0):
        g = affine[0:1, :]
        b = affine[1:2, :]
        start, size = blocks[i]
        step = fitting(NORM_ROWS, size)

        def one(n, carry):
            r = pl.ds(pl.multiple_of(start + n * step, step), step)
            if source is not None:
                values = source[r, :].astype(jnp.float32)
            elif t or i == 0:
                values = xs[t, r, :].astype(jnp.float32)
            else:
                values = pick(t, [slots[k, r, :].astype(jnp.float32) for k in range(n_slots)])
                xs[t, r, :] = values.astype(jnp.bfloat16)
            centred = values - jnp.mean(values, axis=-1, keepdims=True)
            spread = jnp.mean(centred * centred, axis=-1, keepdims=True)
            hs[t, d, r, :] = (centred * lax.rsqrt(spread + EPS) * g + b).astype(jnp.bfloat16)
            return carry

        lax.fori_loop(0, size // step, one, 0, unroll=size // step)

    def project(t):
        for i in range(n_tiles):
            if t == 0:
                wi_copy(i).wait()
            cols = pl.ds(i * wi_tile, wi_tile)
            y = jnp.dot(hs[t, 0], wi[:, cols], preferred_element_type=jnp.float32)
            qkv[0:rows, cols] = y.astype(jnp.bfloat16)

    def project_chunk(t, d, c):
        for i in range(n_tiles):
            cols = pl.ds(i * wi_tile, wi_tile)
            y = jnp.dot(
                hs[t, d, :, span(c)], wi[span(c), cols], preferred_element_type=jnp.float32
            )
            if c:
                y = acc[:, cols] + y
            if c + 1 < n_chunks:
                acc[:, cols] = y
            else:
                qkv[d * rows:(d + 1) * rows, cols] = y.astype(jnp.bfloat16)

    scale = math.log2(math.e) / math.sqrt(HD)

    def attend(t, d):
        r = slice(d * rows, (d + 1) * rows)
        for n in range(heads):
            base = n * 3 * HD
            q = qkv[r, base:base + HD]
            k = qkv[:, base + HD:base + 2 * HD]
            v = qkv[:, base + 2 * HD:base + 3 * HD]
            s = lax.dot_general(q, k, (((1,), (1,)), ((), ())), preferred_element_type=jnp.float32)
            e = jnp.exp2((s - jnp.max(s, axis=-1, keepdims=True)) * scale)
            total = jnp.sum(e, axis=-1, keepdims=True)
            y = jnp.dot(e.astype(jnp.bfloat16), v, preferred_element_type=jnp.float32)
            mixed[:, n * HD:(n + 1) * HD] = (y / total).astype(jnp.bfloat16)

        ready = 0
        for j in range(width // wo_tile):
            cols = pl.ds(j * wo_tile, wo_tile)
            with jax.named_scope(f"wo_{t}_{d}_{j}"):
                y = jnp.dot(mixed[...], wo[:, cols], preferred_element_type=jnp.float32)
                part[t, d, :, cols] = y.astype(jnp.bfloat16)
                if d == 1 and j == 0:
                    @pl.when(late)
                    def _():
                        await_turn(1 + 2 * t)
                while d and ready < len(parts[t]) and sum(parts[t][ready]) <= (j + 1) * wo_tile:
                    rs_copy(t, d, ready).start()
                    ready += 1
        if t + 1 == ticks:
            @pl.when(leads)
            def _():
                copies = shared(t)
                for copy in [copies[1 + d]] if d else copies[:2]:
                    copy.start()

    def hops(t, c):
        return has_next & late if t + 1 == ticks and c == both else has_next

    def finish(t, c):
        with jax.named_scope(f"rs_wait_{t}_{c}"):
            for d in range(1, peers):
                rs_copy(t, d, c).wait_recv()
        if t == 0 and c == min(1, len(parts[t]) - 1):
            yield_turn(1, leads)

        def step(r):
            total = part[t, 0, r, part_span(t, c)].astype(jnp.float32)
            for d in range(1, peers):
                total = total + got[t, d - 1, r, part_span(t, c)].astype(jnp.float32)
            x = xs[t, r, part_span(t, c)].astype(jnp.float32)
            out[t, 0, r, part_span(t, c)] = (x + total).astype(jnp.bfloat16)

        pieces(step)

        @pl.when(hops(t, c))
        def _():
            hop_copy(t, c).start()

    def take(t, c):
        chosen = order[0, t]
        last = t + 1 == ticks

        def step(r, source):
            if source is duo:
                total = duo[1, r, :].astype(jnp.float32)
                for d in range(1, peers):
                    total = total + duo[1 + d, r, :].astype(jnp.float32)
                new = (duo[0, r, :].astype(jnp.float32) + total).astype(jnp.bfloat16)
                new = new.astype(jnp.float32)
            else:
                new = source[t, r, part_span(t, c)].astype(jnp.float32)
            values = [
                jnp.where(chosen == k, new, slots[k, r, part_span(t, c)].astype(jnp.float32))
                for k in range(n_slots)
            ]
            for k in range(n_slots):
                if last:
                    held[0, k, r, part_span(t, c)] = values[k].astype(jnp.bfloat16)
                else:
                    slots[k, r, part_span(t, c)] = values[k].astype(jnp.bfloat16)
            if not last:
                xs[t + 1, r, part_span(t, c)] = pick(t + 1, values).astype(jnp.bfloat16)

        if last and c == both:
            @pl.when(late)
            def _():
                with jax.named_scope("shared_wait"):
                    shared_wait(1)
                pieces(functools.partial(step, source=duo))

            by_hop = has_prev & early
        else:
            by_hop = has_prev

        @pl.when(by_hop)
        def _():
            with jax.named_scope(f"hop_wait_{t}_{c}"):
                hop_copy(t, c).wait_recv()
            pieces(functools.partial(step, source=arr))

        @pl.when(jnp.logical_not(has_prev))
        def _():
            pieces(functools.partial(step, source=fresh_v))

    def first_rows(i):
        with jax.named_scope(f"acts_wait_{i}"):
            acts_copy(i).wait()
            if i == last_block:
                for n in range(n_tiles):
                    wi_copy(n).start()
                load_wo.start()
                load_fresh.start()
        with jax.named_scope(f"norm_first_{i}"):
            if i:
                norm(0, i)
            else:
                offer(i)

    with jax.named_scope("small_wait"):
        load_order.wait()
        pltpu.make_async_copy(affine, affine, small_sem.at[1]).wait()
    first_rows(0)
    with jax.named_scope("barrier"):
        pl.semaphore_wait(
            barrier,
            (peers - 1) * (1 + leads.astype(jnp.int32))
            + has_prev.astype(jnp.int32) + has_next.astype(jnp.int32),
        )
    for i in range(len(blocks)):
        if i:
            first_rows(i)

        @pl.when(early)
        def _():
            send_rows(0, i)

    norm(0, 0)

    with jax.named_scope("project_first"):
        project(0)

    @pl.when(late)
    def _():
        await_turn(0)
        for i in range(len(blocks)):
            send_rows(0, i)

    yield_turn(0, leads)

    for t in range(ticks):
        if t:
            with jax.named_scope(f"lead_{t}"):
                for d in range(1, peers):
                    sent(t, d, 0)

            yield_turn(3, leads)
            yield_turn(2, late)
            reduced(t - 1)
        for d in range(1, peers):
            if t == 0:
                with jax.named_scope("raw_wait"):
                    raw_copy(d).wait_recv()
                with jax.named_scope("raw_norm"):
                    norm(0, 0, raw.at[d - 1], d)
            for c in range(n_chunks):
                with jax.named_scope(f"ag_wait_{t}_{c}"):
                    ag_copy(t, d, c, slice(None) if t else row_block(last_block)).wait_recv()
                with jax.named_scope(f"pchunk_{t}_{c}"):
                    project_chunk(t, d, c)
        if t == 0:
            load_wo.wait()
        for d in [*range(1, peers), 0]:
            with jax.named_scope(f"attend_{t}_{d}"):
                attend(t, d)
        if t == 0:
            load_fresh.wait()
        if t + 1 == ticks:
            if t:
                hopped(t - 1)
            for c in range(len(parts[t])):
                finish(t, c)
            for c in range(len(parts[t])):
                take(t, c)
        else:
            ahead = max(len(parts[t]) - 3, 0)

            @pl.when(early)
            def _():
                for c in range(len(parts[t])):
                    finish(t, c)
                for c in range(len(parts[t])):
                    take(t, c)

            @pl.when(late)
            def _():
                for c in range(len(parts[t])):
                    take(t, c)
                    if 0 <= c - 2 < ahead:
                        finish(t, c - 2)

            gathered(t)
            for i in range(len(blocks)):
                with jax.named_scope(f"norm_{t}_{i}"):
                    norm(t + 1, i)
                if i == 0:
                    @pl.when(leads)
                    def _():
                        await_turn(2)

                send_rows(t + 1, i)

            @pl.when(late)
            def _():
                for c in range(ahead, len(parts[t])):
                    finish(t, c)

            with jax.named_scope(f"project_{t}"):
                project(t + 1)

    gathered(ticks - 1)
    reduced(ticks - 1)
    hopped(ticks - 1)


def flush(out_v, held_v, out, held, sem):
    copies = [
        pltpu.make_async_copy(out_v, out, sem.at[0]),
        pltpu.make_async_copy(held_v, held, sem.at[1]),
    ]
    for copy in copies:
        copy.start()
    for copy in copies:
        copy.wait()


def pin(*xs):
    return [pltpu.with_memory_space_constraint(x, pltpu.HBM) for x in xs]


def body(acts, fresh, order, ln_gain, ln_bias, wqkv, wo):
    ticks, rows, width = fresh.shape
    n_slots = acts.shape[1]
    peers = lax.axis_size("tensor")
    seq = rows * peers
    n_chunks = len(ag_spans(width))
    n_parts = len(rs_spans(width))
    inner = wo.shape[1]
    wide = wqkv.shape[2]
    bf = jnp.bfloat16
    dma = pltpu.SemaphoreType.DMA
    anywhere = pl.BlockSpec(memory_space=pl.ANY)
    vmem = pl.BlockSpec(memory_space=pltpu.VMEM)
    out_shape = (ticks, 1, rows, width)
    held_shape = (1, n_slots, rows, width)
    results = pl.pallas_call(
        relay,
        out_shape=(pltpu.VMEM(out_shape, bf), pltpu.VMEM(held_shape, bf)),
        in_specs=[anywhere] * 7,
        out_specs=(vmem, vmem),
        scratch_shapes=[
            pltpu.SMEM(order.shape, jnp.int32),
            pltpu.VMEM((2, width), jnp.float32),
            pltpu.VMEM((n_slots, rows, width), bf),
            pltpu.VMEM((ticks, rows, width), bf),
            pltpu.VMEM((width, wide), bf),
            pltpu.VMEM((inner, width), bf),
            pltpu.VMEM((ticks, rows, width), bf),
            pltpu.VMEM((ticks, peers, rows, width), bf),
            pltpu.VMEM((rows, wide), jnp.float32),
            pltpu.VMEM((seq, wide), bf),
            pltpu.VMEM((rows, inner), bf),
            pltpu.VMEM((ticks, peers, rows, width), bf),
            pltpu.VMEM((ticks, peers - 1, rows, width), bf),
            pltpu.VMEM((ticks, rows, width), bf),
            pltpu.VMEM((peers + 1, rows, rs_spans(width)[-1][1]), bf),
            pltpu.VMEM((peers - 1, rows // 4, width), bf),
            dma((2,)),
            dma((2,)),
            dma,
            dma((wide // fitting(TILE, wide),)),
            dma,
            dma((peers - 1, 2)),
            dma((ticks, peers - 1, n_chunks)),
            dma((peers - 1,)),
            dma((ticks, peers - 1, n_parts)),
            dma,
            dma((ticks, n_parts)),
            dma((2,)),
            dma((peers - 1,)),
            pltpu.SemaphoreType.REGULAR((1,)),
        ],
        compiler_params=pltpu.CompilerParams(
            collective_id=0, has_side_effects=True, vmem_limit_bytes=52 * 1024 * 1024
        ),
    )(*pin(acts, fresh, order, ln_gain, ln_bias, wqkv, wo))
    return pl.pallas_call(
        flush,
        out_shape=(jax.ShapeDtypeStruct(out_shape, bf), jax.ShapeDtypeStruct(held_shape, bf)),
        in_specs=[vmem, vmem],
        out_specs=(pl.BlockSpec(memory_space=pltpu.HBM), pl.BlockSpec(memory_space=pltpu.HBM)),
        scratch_shapes=[dma((2,))],
    )(*[pltpu.with_memory_space_constraint(x, pltpu.VMEM) for x in results])


def solution(mesh):
    return jax.shard_map(
        body,
        mesh=mesh,
        in_specs=(
            P("section", "dp", "tensor", None),
            P("dp", "tensor", None),
            P("section", None),
            P("section", None),
            P("section", None),
            P("section", None, "tensor"),
            P("section", "tensor", None),
        ),
        out_specs=(P("dp", "section", "tensor", None), P("section", "dp", "tensor", None)),
        check_vma=False,
    )
```

```python
import functools
import math

import jax
import jax.numpy as jnp
from jax import lax
from jax.experimental import pallas as pl
from jax.experimental.pallas import tpu as pltpu
from jax.sharding import PartitionSpec as P

HD = 128
EPS = 1e-06
CHUNK = 512
TILE = 1024
NORM_ROWS = 16
PIECE = 32
MESH = pl.DeviceIdType.MESH


def fitting(most, size):
    return math.gcd(most, size)


def spans(sizes):
    return [(sum(sizes[:i]), size) for i, size in enumerate(sizes)]


def ag_spans(width):
    chunk = fitting(CHUNK, width)
    half = chunk // 2
    if width < 2 * chunk:
        return spans([chunk])
    return spans([chunk + half] + [chunk] * (width // chunk - 2) + [half])


def rs_spans(width):
    chunk = fitting(CHUNK, width)
    half = chunk // 2
    return spans([chunk] * (width // chunk - 1) + [half, half])


def relay(
    acts, fresh, order_h, gain_h, bias_h, w_in, w_out, out, held,
    order, affine, slots, fresh_v, wi, wo, xs, hs, acc, qkv, mixed, part, got, arr, duo, raw,
    small_sem, acts_sem, fresh_sem, wi_sem, wo_sem,
    ag_send, ag_recv, rs_send, rs_recv, hop_send, hop_recv, duo_sem, raw_sem, turn,
):
    ticks, rows, width = fresh.shape
    n_slots = acts.shape[1]
    peers = lax.axis_size("tensor")
    sections = lax.axis_size("section")
    me = lax.axis_index("tensor")
    sec = lax.axis_index("section")
    heads = wi.shape[1] // (3 * HD)
    wi_tile = fitting(TILE, wi.shape[1])
    n_tiles = wi.shape[1] // wi_tile
    has_prev = sec > 0
    has_next = sec < sections - 1
    late = lax.rem(sec, 2) == 1
    early = jnp.logical_not(late)
    leads = early & has_next
    chunks = ag_spans(width)
    n_chunks = len(chunks)
    parts = [rs_spans(width) for t in range(ticks)]
    both = len(parts[-1]) - 1
    wo_tile = fitting(CHUNK, width)
    blocks = spans([rows // 4, rows - rows // 4])
    last_block = len(blocks) - 1

    def span(c):
        return pl.ds(*chunks[c])

    def part_span(t, c):
        return pl.ds(*parts[t][c])

    barrier = pltpu.get_barrier_semaphore()
    for d in range(1, peers):
        pl.semaphore_signal(
            barrier, inc=1, device_id={"tensor": lax.rem(me + d, peers)}, device_id_type=MESH
        )

    @pl.when(has_prev)
    def _():
        pl.semaphore_signal(barrier, inc=1, device_id={"section": sec - 1}, device_id_type=MESH)

    @pl.when(late)
    def _():
        for d in range(1, peers):
            pl.semaphore_signal(
                barrier, inc=1,
                device_id={"tensor": lax.rem(me + d, peers), "section": sec - 1},
                device_id_type=MESH,
            )

    @pl.when(has_next)
    def _():
        pl.semaphore_signal(barrier, inc=1, device_id={"section": sec + 1}, device_id_type=MESH)

    def row_block(i):
        return pl.ds(*blocks[i])

    def acts_copy(i):
        return pltpu.make_async_copy(
            acts.at[0, :, row_block(i)], slots.at[:, row_block(i)], acts_sem.at[i]
        )

    load_order = pltpu.make_async_copy(order_h, order, small_sem.at[0])
    load_order.start()
    acts_copy(0).start()
    pltpu.make_async_copy(gain_h, affine.at[0:1], small_sem.at[1]).start()
    pltpu.make_async_copy(bias_h, affine.at[1:2], small_sem.at[1]).start()
    for i in range(1, len(blocks)):
        acts_copy(i).start()

    def wi_copy(i):
        cols = pl.ds(i * wi_tile, wi_tile)
        return pltpu.make_async_copy(w_in.at[0, :, cols], wi.at[:, cols], wi_sem.at[i])

    load_wo = pltpu.make_async_copy(w_out.at[0], wo, wo_sem)
    load_fresh = pltpu.make_async_copy(fresh, fresh_v, fresh_sem)

    def ag_copy(t, d, c, r=slice(None), tail=0):
        return pltpu.make_async_remote_copy(
            src_ref=hs.at[t, 0, r, span(c)],
            dst_ref=hs.at[t, d, r, span(c)],
            send_sem=ag_send.at[d - 1, tail],
            recv_sem=ag_recv.at[t, d - 1, c],
            device_id={"tensor": lax.rem(me + d, peers)},
            device_id_type=MESH,
        )

    def rs_copy(t, d, c):
        return pltpu.make_async_remote_copy(
            src_ref=part.at[t, d, :, part_span(t, c)],
            dst_ref=got.at[t, d - 1, :, part_span(t, c)],
            send_sem=rs_send.at[d - 1],
            recv_sem=rs_recv.at[t, d - 1, c],
            device_id={"tensor": lax.rem(me - d + peers, peers)},
            device_id_type=MESH,
        )

    def hop_copy(t, c):
        return pltpu.make_async_remote_copy(
            src_ref=out.at[t, 0, :, part_span(t, c)],
            dst_ref=arr.at[t, :, part_span(t, c)],
            send_sem=hop_send,
            recv_sem=hop_recv.at[t, c],
            device_id={"section": lax.rem(sec + 1, sections)},
            device_id_type=MESH,
        )

    def shared(t):
        cols = part_span(t, both)
        sources = [xs.at[t, :, cols]] + [part.at[t, d, :, cols] for d in range(peers)]
        return [
            pltpu.make_async_remote_copy(
                src_ref=source,
                dst_ref=duo.at[i],
                send_sem=duo_sem.at[0],
                recv_sem=duo_sem.at[1],
                device_id={
                    "tensor": lax.rem(me - max(i - 1, 0) + peers, peers),
                    "section": lax.rem(sec + 1, sections),
                },
                device_id_type=MESH,
            )
            for i, source in enumerate(sources)
        ]

    def shared_wait(i):
        pltpu.make_async_copy(duo, duo, duo_sem.at[i]).wait()

    def yield_turn(i, when):
        partner = sec + 1 - 2 * lax.rem(sec, 2)

        @pl.when(when)
        def _():
            pl.semaphore_signal(
                turn.at[0], inc=1, device_id={"section": partner}, device_id_type=MESH
            )

    def await_turn(i):
        with jax.named_scope(f"turn_{i}"):
            pl.semaphore_wait(turn.at[0], 1)

    def pieces(step):
        for i in range(rows // PIECE):
            step(pl.ds(i * PIECE, PIECE))

    def pick(t, values):
        chosen = order[0, t]
        x = values[0]
        for k in range(1, n_slots):
            x = jnp.where(chosen == k, values[k], x)
        return x

    n_lead = max(1, n_chunks - 2)
    lead_cols = sum(size for _, size in chunks[:n_lead])

    def raw_copy(d):
        return pltpu.make_async_remote_copy(
            src_ref=xs.at[0, row_block(0)],
            dst_ref=raw.at[d - 1],
            send_sem=ag_send.at[d - 1, 0],
            recv_sem=raw_sem.at[d - 1],
            device_id={"tensor": lax.rem(me + d, peers)},
            device_id_type=MESH,
        )

    def send_rows(t, i):
        if t == 0 and i == 0:
            for d in range(1, peers):
                raw_copy(d).start()
            return
        for c in range(n_chunks):
            for d in range(1, peers):
                ag_copy(t, d, c, row_block(i), int(i == last_block and c >= n_lead)).start()

    def sent(t, d, tail):
        def drain(r, cols):
            copied = hs.at[t, 0, r, cols]
            pltpu.make_async_copy(copied, copied, ag_send.at[d - 1, tail]).wait()

        if tail:
            if lead_cols < width:
                drain(row_block(last_block), pl.ds(lead_cols, width - lead_cols))
        else:
            for i in range(last_block):
                drain(row_block(i), pl.ds(0, width))
            drain(row_block(last_block), pl.ds(0, lead_cols))

    def gathered(t):
        for d in range(1, peers):
            if t == 0:
                sent(t, d, 0)
            sent(t, d, 1)

    def reduced(t):
        for d in range(1, peers):
            pltpu.make_async_copy(hs.at[t, 0], hs.at[t, 0], rs_send.at[d - 1]).wait()

    def hopped(t):
        def drain(cols):
            copied = hs.at[t, 0, :, cols]
            pltpu.make_async_copy(copied, copied, hop_send).wait()

        if t + 1 < ticks:
            @pl.when(has_next)
            def _():
                drain(pl.ds(0, width))
        else:
            @pl.when(has_next & late)
            def _():
                drain(pl.ds(0, width))

            @pl.when(leads)
            def _():
                drain(pl.ds(0, parts[t][both][0]))
                shared_wait(0)

    def offer(i):
        start, size = blocks[i]
        for n in range(size // PIECE):
            r = pl.ds(start + n * PIECE, PIECE)
            values = pick(0, [slots[k, r, :].astype(jnp.float32) for k in range(n_slots)])
            xs[0, r, :] = values.astype(jnp.bfloat16)

    def norm(t, i, source=None, d=0):
        g = affine[0:1, :]
        b = affine[1:2, :]
        start, size = blocks[i]
        step = fitting(NORM_ROWS, size)

        def one(n, carry):
            r = pl.ds(pl.multiple_of(start + n * step, step), step)
            if source is not None:
                values = source[r, :].astype(jnp.float32)
            elif t or i == 0:
                values = xs[t, r, :].astype(jnp.float32)
            else:
                values = pick(t, [slots[k, r, :].astype(jnp.float32) for k in range(n_slots)])
                xs[t, r, :] = values.astype(jnp.bfloat16)
            centred = values - jnp.mean(values, axis=-1, keepdims=True)
            spread = jnp.mean(centred * centred, axis=-1, keepdims=True)
            hs[t, d, r, :] = (centred * lax.rsqrt(spread + EPS) * g + b).astype(jnp.bfloat16)
            return carry

        lax.fori_loop(0, size // step, one, 0, unroll=size // step)

    def project(t):
        for i in range(n_tiles):
            if t == 0:
                wi_copy(i).wait()
            cols = pl.ds(i * wi_tile, wi_tile)
            y = jnp.dot(hs[t, 0], wi[:, cols], preferred_element_type=jnp.float32)
            qkv[0:rows, cols] = y.astype(jnp.bfloat16)

    def project_chunk(t, d, c):
        for i in range(n_tiles):
            cols = pl.ds(i * wi_tile, wi_tile)
            y = jnp.dot(
                hs[t, d, :, span(c)], wi[span(c), cols], preferred_element_type=jnp.float32
            )
            if c:
                y = acc[:, cols] + y
            if c + 1 < n_chunks:
                acc[:, cols] = y
            else:
                qkv[d * rows:(d + 1) * rows, cols] = y.astype(jnp.bfloat16)

    scale = math.log2(math.e) / math.sqrt(HD)

    def attend(t, d):
        r = slice(d * rows, (d + 1) * rows)
        for n in range(heads):
            base = n * 3 * HD
            q = qkv[r, base:base + HD]
            k = qkv[:, base + HD:base + 2 * HD]
            v = qkv[:, base + 2 * HD:base + 3 * HD]
            s = lax.dot_general(q, k, (((1,), (1,)), ((), ())), preferred_element_type=jnp.float32)
            e = jnp.exp2((s - jnp.max(s, axis=-1, keepdims=True)) * scale)
            total = jnp.sum(e, axis=-1, keepdims=True)
            y = jnp.dot(e.astype(jnp.bfloat16), v, preferred_element_type=jnp.float32)
            mixed[:, n * HD:(n + 1) * HD] = (y / total).astype(jnp.bfloat16)

        ready = 0
        for j in range(width // wo_tile):
            cols = pl.ds(j * wo_tile, wo_tile)
            with jax.named_scope(f"wo_{t}_{d}_{j}"):
                y = jnp.dot(mixed[...], wo[:, cols], preferred_element_type=jnp.float32)
                part[t, d, :, cols] = y.astype(jnp.bfloat16)
                if d == 1 and j == 0:
                    @pl.when(late)
                    def _():
                        await_turn(1 + 2 * t)
                while d and ready < len(parts[t]) and sum(parts[t][ready]) <= (j + 1) * wo_tile:
                    rs_copy(t, d, ready).start()
                    ready += 1
        if t + 1 == ticks:
            @pl.when(leads)
            def _():
                copies = shared(t)
                for copy in [copies[1 + d]] if d else copies[:2]:
                    copy.start()

    def hops(t, c):
        return has_next & late if t + 1 == ticks and c == both else has_next

    def finish(t, c):
        with jax.named_scope(f"rs_wait_{t}_{c}"):
            for d in range(1, peers):
                rs_copy(t, d, c).wait_recv()
        if t == 0 and c == min(1, len(parts[t]) - 1):
            yield_turn(1, leads)

        def step(r):
            total = part[t, 0, r, part_span(t, c)].astype(jnp.float32)
            for d in range(1, peers):
                total = total + got[t, d - 1, r, part_span(t, c)].astype(jnp.float32)
            x = xs[t, r, part_span(t, c)].astype(jnp.float32)
            out[t, 0, r, part_span(t, c)] = (x + total).astype(jnp.bfloat16)

        pieces(step)

        @pl.when(hops(t, c))
        def _():
            hop_copy(t, c).start()

    def take(t, c):
        chosen = order[0, t]
        last = t + 1 == ticks

        def step(r, source):
            if source is duo:
                total = duo[1, r, :].astype(jnp.float32)
                for d in range(1, peers):
                    total = total + duo[1 + d, r, :].astype(jnp.float32)
                new = (duo[0, r, :].astype(jnp.float32) + total).astype(jnp.bfloat16)
                new = new.astype(jnp.float32)
            else:
                new = source[t, r, part_span(t, c)].astype(jnp.float32)
            values = [
                jnp.where(chosen == k, new, slots[k, r, part_span(t, c)].astype(jnp.float32))
                for k in range(n_slots)
            ]
            for k in range(n_slots):
                if last:
                    held[0, k, r, part_span(t, c)] = values[k].astype(jnp.bfloat16)
                else:
                    slots[k, r, part_span(t, c)] = values[k].astype(jnp.bfloat16)
            if not last:
                xs[t + 1, r, part_span(t, c)] = pick(t + 1, values).astype(jnp.bfloat16)

        if last and c == both:
            @pl.when(late)
            def _():
                with jax.named_scope("shared_wait"):
                    shared_wait(1)
                pieces(functools.partial(step, source=duo))

            by_hop = has_prev & early
        else:
            by_hop = has_prev

        @pl.when(by_hop)
        def _():
            with jax.named_scope(f"hop_wait_{t}_{c}"):
                hop_copy(t, c).wait_recv()
            pieces(functools.partial(step, source=arr))

        @pl.when(jnp.logical_not(has_prev))
        def _():
            pieces(functools.partial(step, source=fresh_v))

    def first_rows(i):
        with jax.named_scope(f"acts_wait_{i}"):
            acts_copy(i).wait()
            if i == last_block:
                for n in range(n_tiles):
                    wi_copy(n).start()
                load_wo.start()
                load_fresh.start()
        with jax.named_scope(f"norm_first_{i}"):
            if i:
                norm(0, i)
            else:
                offer(i)

    with jax.named_scope("small_wait"):
        load_order.wait()
        pltpu.make_async_copy(affine, affine, small_sem.at[1]).wait()
    first_rows(0)
    with jax.named_scope("barrier"):
        pl.semaphore_wait(
            barrier,
            (peers - 1) * (1 + leads.astype(jnp.int32))
            + has_prev.astype(jnp.int32) + has_next.astype(jnp.int32),
        )
    for i in range(len(blocks)):
        if i:
            first_rows(i)

        @pl.when(early)
        def _():
            send_rows(0, i)

    norm(0, 0)

    with jax.named_scope("project_first"):
        project(0)

    @pl.when(late)
    def _():
        await_turn(0)
        for i in range(len(blocks)):
            send_rows(0, i)

    yield_turn(0, leads)

    for t in range(ticks):
        if t:
            with jax.named_scope(f"lead_{t}"):
                for d in range(1, peers):
                    sent(t, d, 0)

            yield_turn(3, leads)
            yield_turn(2, late)
            reduced(t - 1)
        for d in range(1, peers):
            if t == 0:
                with jax.named_scope("raw_wait"):
                    raw_copy(d).wait_recv()
                with jax.named_scope("raw_norm"):
                    norm(0, 0, raw.at[d - 1], d)
            for c in range(n_chunks):
                with jax.named_scope(f"ag_wait_{t}_{c}"):
                    ag_copy(t, d, c, slice(None) if t else row_block(last_block)).wait_recv()
                with jax.named_scope(f"pchunk_{t}_{c}"):
                    project_chunk(t, d, c)
        if t == 0:
            load_wo.wait()
        for d in [*range(1, peers), 0]:
            with jax.named_scope(f"attend_{t}_{d}"):
                attend(t, d)
        if t == 0:
            load_fresh.wait()
        if t + 1 == ticks:
            if t:
                hopped(t - 1)

            @pl.when(early)
            def _():
                for c in range(both):
                    finish(t, c)
                for c in range(len(parts[t])):
                    take(t, c)
                finish(t, both)

            @pl.when(late)
            def _():
                for c in range(len(parts[t])):
                    finish(t, c)
                for c in range(len(parts[t])):
                    take(t, c)
        else:
            ahead = max(len(parts[t]) - 3, 0)

            @pl.when(early)
            def _():
                for c in range(len(parts[t])):
                    finish(t, c)
                for c in range(len(parts[t])):
                    take(t, c)

            @pl.when(late)
            def _():
                for c in range(len(parts[t])):
                    take(t, c)
                    if 0 <= c - 2 < ahead:
                        finish(t, c - 2)

            gathered(t)
            for i in range(len(blocks)):
                with jax.named_scope(f"norm_{t}_{i}"):
                    norm(t + 1, i)
                if i == 0:
                    @pl.when(leads)
                    def _():
                        await_turn(2)

                send_rows(t + 1, i)

            @pl.when(late)
            def _():
                for c in range(ahead, len(parts[t])):
                    finish(t, c)

            with jax.named_scope(f"project_{t}"):
                project(t + 1)

    gathered(ticks - 1)
    reduced(ticks - 1)
    hopped(ticks - 1)


def flush(out_v, held_v, out, held, sem):
    copies = [
        pltpu.make_async_copy(out_v, out, sem.at[0]),
        pltpu.make_async_copy(held_v, held, sem.at[1]),
    ]
    for copy in copies:
        copy.start()
    for copy in copies:
        copy.wait()


def pin(*xs):
    return [pltpu.with_memory_space_constraint(x, pltpu.HBM) for x in xs]


def body(acts, fresh, order, ln_gain, ln_bias, wqkv, wo):
    ticks, rows, width = fresh.shape
    n_slots = acts.shape[1]
    peers = lax.axis_size("tensor")
    seq = rows * peers
    n_chunks = len(ag_spans(width))
    n_parts = len(rs_spans(width))
    inner = wo.shape[1]
    wide = wqkv.shape[2]
    bf = jnp.bfloat16
    dma = pltpu.SemaphoreType.DMA
    anywhere = pl.BlockSpec(memory_space=pl.ANY)
    vmem = pl.BlockSpec(memory_space=pltpu.VMEM)
    out_shape = (ticks, 1, rows, width)
    held_shape = (1, n_slots, rows, width)
    results = pl.pallas_call(
        relay,
        out_shape=(pltpu.VMEM(out_shape, bf), pltpu.VMEM(held_shape, bf)),
        in_specs=[anywhere] * 7,
        out_specs=(vmem, vmem),
        scratch_shapes=[
            pltpu.SMEM(order.shape, jnp.int32),
            pltpu.VMEM((2, width), jnp.float32),
            pltpu.VMEM((n_slots, rows, width), bf),
            pltpu.VMEM((ticks, rows, width), bf),
            pltpu.VMEM((width, wide), bf),
            pltpu.VMEM((inner, width), bf),
            pltpu.VMEM((ticks, rows, width), bf),
            pltpu.VMEM((ticks, peers, rows, width), bf),
            pltpu.VMEM((rows, wide), jnp.float32),
            pltpu.VMEM((seq, wide), bf),
            pltpu.VMEM((rows, inner), bf),
            pltpu.VMEM((ticks, peers, rows, width), bf),
            pltpu.VMEM((ticks, peers - 1, rows, width), bf),
            pltpu.VMEM((ticks, rows, width), bf),
            pltpu.VMEM((peers + 1, rows, rs_spans(width)[-1][1]), bf),
            pltpu.VMEM((peers - 1, rows // 4, width), bf),
            dma((2,)),
            dma((2,)),
            dma,
            dma((wide // fitting(TILE, wide),)),
            dma,
            dma((peers - 1, 2)),
            dma((ticks, peers - 1, n_chunks)),
            dma((peers - 1,)),
            dma((ticks, peers - 1, n_parts)),
            dma,
            dma((ticks, n_parts)),
            dma((2,)),
            dma((peers - 1,)),
            pltpu.SemaphoreType.REGULAR((1,)),
        ],
        compiler_params=pltpu.CompilerParams(
            collective_id=0, has_side_effects=True, vmem_limit_bytes=52 * 1024 * 1024
        ),
    )(*pin(acts, fresh, order, ln_gain, ln_bias, wqkv, wo))
    return pl.pallas_call(
        flush,
        out_shape=(jax.ShapeDtypeStruct(out_shape, bf), jax.ShapeDtypeStruct(held_shape, bf)),
        in_specs=[vmem, vmem],
        out_specs=(pl.BlockSpec(memory_space=pltpu.HBM), pl.BlockSpec(memory_space=pltpu.HBM)),
        scratch_shapes=[dma((2,))],
    )(*[pltpu.with_memory_space_constraint(x, pltpu.VMEM) for x in results])


def solution(mesh):
    return jax.shard_map(
        body,
        mesh=mesh,
        in_specs=(
            P("section", "dp", "tensor", None),
            P("dp", "tensor", None),
            P("section", None),
            P("section", None),
            P("section", None),
            P("section", None, "tensor"),
            P("section", "tensor", None),
        ),
        out_specs=(P("dp", "section", "tensor", None), P("section", "dp", "tensor", None)),
        check_vma=False,
    )
```

```python
import functools
import math

import jax
import jax.numpy as jnp
from jax import lax
from jax.experimental import pallas as pl
from jax.experimental.pallas import tpu as pltpu
from jax.sharding import PartitionSpec as P

HD = 128
EPS = 1e-06
CHUNK = 512
TILE = 1024
NORM_ROWS = 16
PIECE = 32
MESH = pl.DeviceIdType.MESH


def fitting(most, size):
    return math.gcd(most, size)


def spans(sizes):
    return [(sum(sizes[:i]), size) for i, size in enumerate(sizes)]


def ag_spans(width):
    chunk = fitting(CHUNK, width)
    half = chunk // 2
    if width < 2 * chunk:
        return spans([chunk])
    return spans([chunk + half] + [chunk] * (width // chunk - 2) + [half])


def rs_spans(width):
    chunk = fitting(CHUNK, width)
    half = chunk // 2
    return spans([chunk] * (width // chunk - 1) + [half, half])


def relay(
    acts, fresh, order_h, gain_h, bias_h, w_in, w_out, out, held,
    order, affine, slots, fresh_v, wi, wo, xs, hs, acc, qkv, mixed, part, got, arr, duo, raw,
    small_sem, acts_sem, fresh_sem, wi_sem, wo_sem,
    ag_send, ag_recv, rs_send, rs_recv, hop_recv, duo_sem, raw_sem, turn,
):
    ticks, rows, width = fresh.shape
    n_slots = acts.shape[1]
    peers = lax.axis_size("tensor")
    sections = lax.axis_size("section")
    me = lax.axis_index("tensor")
    sec = lax.axis_index("section")
    heads = wi.shape[1] // (3 * HD)
    wi_tile = fitting(TILE, wi.shape[1])
    n_tiles = wi.shape[1] // wi_tile
    has_prev = sec > 0
    has_next = sec < sections - 1
    late = lax.rem(sec, 2) == 1
    early = jnp.logical_not(late)
    leads = early & has_next
    chunks = ag_spans(width)
    n_chunks = len(chunks)
    parts = [rs_spans(width) for t in range(ticks)]
    both = len(parts[-1]) - 1
    wo_tile = fitting(CHUNK, width)
    blocks = spans([rows // 8, rows - rows // 8])
    last_block = len(blocks) - 1

    def span(c):
        return pl.ds(*chunks[c])

    def part_span(t, c):
        return pl.ds(*parts[t][c])

    barrier = pltpu.get_barrier_semaphore()
    for d in range(1, peers):
        pl.semaphore_signal(
            barrier, inc=1, device_id={"tensor": lax.rem(me + d, peers)}, device_id_type=MESH
        )

    @pl.when(has_prev)
    def _():
        pl.semaphore_signal(barrier, inc=1, device_id={"section": sec - 1}, device_id_type=MESH)

    @pl.when(late)
    def _():
        for d in range(1, peers):
            pl.semaphore_signal(
                barrier, inc=1,
                device_id={"tensor": lax.rem(me + d, peers), "section": sec - 1},
                device_id_type=MESH,
            )

    @pl.when(has_next)
    def _():
        pl.semaphore_signal(barrier, inc=1, device_id={"section": sec + 1}, device_id_type=MESH)

    def row_block(i):
        return pl.ds(*blocks[i])

    def acts_copy(i):
        return pltpu.make_async_copy(
            acts.at[0, :, row_block(i)], slots.at[:, row_block(i)], acts_sem.at[i]
        )

    load_order = pltpu.make_async_copy(order_h, order, small_sem.at[0])
    load_order.start()
    acts_copy(0).start()
    pltpu.make_async_copy(gain_h, affine.at[0:1], small_sem.at[1]).start()
    pltpu.make_async_copy(bias_h, affine.at[1:2], small_sem.at[1]).start()
    for i in range(1, len(blocks)):
        acts_copy(i).start()

    def wi_copy(i):
        cols = pl.ds(i * wi_tile, wi_tile)
        return pltpu.make_async_copy(w_in.at[0, :, cols], wi.at[:, cols], wi_sem.at[i])

    load_wo = pltpu.make_async_copy(w_out.at[0], wo, wo_sem)
    load_fresh = pltpu.make_async_copy(fresh, fresh_v, fresh_sem)

    def ag_copy(t, d, c, r=slice(None), tail=0):
        return pltpu.make_async_remote_copy(
            src_ref=hs.at[t, 0, r, span(c)],
            dst_ref=hs.at[t, d, r, span(c)],
            send_sem=ag_send.at[d - 1, tail],
            recv_sem=ag_recv.at[t, d - 1, c],
            device_id={"tensor": lax.rem(me + d, peers)},
            device_id_type=MESH,
        )

    def rs_copy(t, d, c):
        return pltpu.make_async_remote_copy(
            src_ref=part.at[t, d, :, part_span(t, c)],
            dst_ref=got.at[t, d - 1, :, part_span(t, c)],
            send_sem=rs_send.at[d - 1],
            recv_sem=rs_recv.at[t, d - 1, c],
            device_id={"tensor": lax.rem(me - d + peers, peers)},
            device_id_type=MESH,
        )

    def hop_copy(t, c):
        return pltpu.make_async_remote_copy(
            src_ref=out.at[t, 0, :, part_span(t, c)],
            dst_ref=arr.at[t, :, part_span(t, c)],
            send_sem=fresh_sem,
            recv_sem=hop_recv.at[t, c],
            device_id={"section": lax.rem(sec + 1, sections)},
            device_id_type=MESH,
        )

    def shared(t):
        cols = part_span(t, both)
        sources = [xs.at[t, :, cols]] + [part.at[t, d, :, cols] for d in range(peers)]
        return [
            pltpu.make_async_remote_copy(
                src_ref=source,
                dst_ref=duo.at[i],
                send_sem=wo_sem,
                recv_sem=duo_sem,
                device_id={
                    "tensor": lax.rem(me - max(i - 1, 0) + peers, peers),
                    "section": lax.rem(sec + 1, sections),
                },
                device_id_type=MESH,
            )
            for i, source in enumerate(sources)
        ]

    def shared_wait(sem):
        pltpu.make_async_copy(duo, duo, sem).wait()

    def yield_turn(i, when):
        partner = sec + 1 - 2 * lax.rem(sec, 2)

        @pl.when(when)
        def _():
            pl.semaphore_signal(
                turn.at[0], inc=1, device_id={"section": partner}, device_id_type=MESH
            )

    def await_turn(i):
        with jax.named_scope(f"turn_{i}"):
            pl.semaphore_wait(turn.at[0], 1)

    def pieces(step):
        for i in range(rows // PIECE):
            step(pl.ds(i * PIECE, PIECE))

    def pick(t, values):
        chosen = order[0, t]
        x = values[0]
        for k in range(1, n_slots):
            x = jnp.where(chosen == k, values[k], x)
        return x

    n_lead = max(1, n_chunks - 2)
    lead_cols = sum(size for _, size in chunks[:n_lead])

    def raw_copy(d):
        return pltpu.make_async_remote_copy(
            src_ref=xs.at[0, row_block(0)],
            dst_ref=raw.at[d - 1],
            send_sem=ag_send.at[d - 1, 0],
            recv_sem=raw_sem.at[d - 1],
            device_id={"tensor": lax.rem(me + d, peers)},
            device_id_type=MESH,
        )

    def send_rows(t, i):
        if t == 0 and i == 0:
            for d in range(1, peers):
                raw_copy(d).start()
            return
        for c in range(n_chunks):
            for d in range(1, peers):
                ag_copy(t, d, c, row_block(i), int(i == last_block and c >= n_lead)).start()

    def sent(t, d, tail):
        def drain(r, cols):
            copied = hs.at[t, 0, r, cols]
            pltpu.make_async_copy(copied, copied, ag_send.at[d - 1, tail]).wait()

        if tail:
            if lead_cols < width:
                drain(row_block(last_block), pl.ds(lead_cols, width - lead_cols))
        else:
            for i in range(last_block):
                drain(row_block(i), pl.ds(0, width))
            drain(row_block(last_block), pl.ds(0, lead_cols))

    def gathered(t):
        for d in range(1, peers):
            if t == 0:
                sent(t, d, 0)
            sent(t, d, 1)

    def reduced(t):
        for d in range(1, peers):
            pltpu.make_async_copy(hs.at[t, 0], hs.at[t, 0], rs_send.at[d - 1]).wait()

    def hopped(t):
        def drain(cols):
            copied = hs.at[t, 0, :, cols]
            pltpu.make_async_copy(copied, copied, fresh_sem).wait()

        if t + 1 < ticks:
            @pl.when(has_next)
            def _():
                drain(pl.ds(0, width))
        else:
            @pl.when(has_next & late)
            def _():
                drain(pl.ds(0, width))

            @pl.when(leads)
            def _():
                drain(pl.ds(0, parts[t][both][0]))
                shared_wait(wo_sem)

    def offer(i):
        start, size = blocks[i]
        piece = fitting(PIECE, size)
        for n in range(size // piece):
            r = pl.ds(start + n * piece, piece)
            values = pick(0, [slots[k, r, :].astype(jnp.float32) for k in range(n_slots)])
            xs[0, r, :] = values.astype(jnp.bfloat16)

    def norm(t, i, source=None, d=0):
        g = affine[0:1, :]
        b = affine[1:2, :]
        start, size = blocks[i]
        step = fitting(NORM_ROWS, size)

        def one(n, carry):
            r = pl.ds(pl.multiple_of(start + n * step, step), step)
            if source is not None:
                values = source[r, :].astype(jnp.float32)
            elif t or i == 0:
                values = xs[t, r, :].astype(jnp.float32)
            else:
                values = pick(t, [slots[k, r, :].astype(jnp.float32) for k in range(n_slots)])
                xs[t, r, :] = values.astype(jnp.bfloat16)
            centred = values - jnp.mean(values, axis=-1, keepdims=True)
            spread = jnp.mean(centred * centred, axis=-1, keepdims=True)
            hs[t, d, r, :] = (centred * lax.rsqrt(spread + EPS) * g + b).astype(jnp.bfloat16)
            return carry

        lax.fori_loop(0, size // step, one, 0, unroll=size // step)

    def project(t):
        for i in range(n_tiles):
            if t == 0:
                wi_copy(i).wait()
            cols = pl.ds(i * wi_tile, wi_tile)
            y = jnp.dot(hs[t, 0], wi[:, cols], preferred_element_type=jnp.float32)
            qkv[0:rows, cols] = y.astype(jnp.bfloat16)

    def project_chunk(t, d, c):
        for i in range(n_tiles):
            cols = pl.ds(i * wi_tile, wi_tile)
            y = jnp.dot(
                hs[t, d, :, span(c)], wi[span(c), cols], preferred_element_type=jnp.float32
            )
            if c:
                y = acc[:, cols] + y
            if c + 1 < n_chunks:
                acc[:, cols] = y
            else:
                qkv[d * rows:(d + 1) * rows, cols] = y.astype(jnp.bfloat16)

    scale = math.log2(math.e) / math.sqrt(HD)

    def attend(t, d):
        r = slice(d * rows, (d + 1) * rows)
        for n in range(heads):
            base = n * 3 * HD
            q = qkv[r, base:base + HD]
            k = qkv[:, base + HD:base + 2 * HD]
            v = qkv[:, base + 2 * HD:base + 3 * HD]
            s = lax.dot_general(q, k, (((1,), (1,)), ((), ())), preferred_element_type=jnp.float32)
            e = jnp.exp2((s - jnp.max(s, axis=-1, keepdims=True)) * scale)
            total = jnp.sum(e, axis=-1, keepdims=True)
            y = jnp.dot(e.astype(jnp.bfloat16), v, preferred_element_type=jnp.float32)
            mixed[:, n * HD:(n + 1) * HD] = (y / total).astype(jnp.bfloat16)

        ready = 0
        for j in range(width // wo_tile):
            cols = pl.ds(j * wo_tile, wo_tile)
            with jax.named_scope(f"wo_{t}_{d}_{j}"):
                y = jnp.dot(mixed[...], wo[:, cols], preferred_element_type=jnp.float32)
                part[t, d, :, cols] = y.astype(jnp.bfloat16)
                if d == 1 and j == 0:
                    @pl.when(late)
                    def _():
                        await_turn(1 + 2 * t)
                while d and ready < len(parts[t]) and sum(parts[t][ready]) <= (j + 1) * wo_tile:
                    rs_copy(t, d, ready).start()
                    ready += 1
        if t + 1 == ticks:
            @pl.when(leads)
            def _():
                copies = shared(t)
                for copy in [copies[1 + d]] if d else copies[:2]:
                    copy.start()

    def hops(t, c):
        return has_next & late if t + 1 == ticks and c == both else has_next

    def finish(t, c):
        with jax.named_scope(f"rs_wait_{t}_{c}"):
            for d in range(1, peers):
                rs_copy(t, d, c).wait_recv()
        if t == 0 and c == min(1, len(parts[t]) - 1):
            yield_turn(1, leads)

        def step(r):
            total = part[t, 0, r, part_span(t, c)].astype(jnp.float32)
            for d in range(1, peers):
                total = total + got[t, d - 1, r, part_span(t, c)].astype(jnp.float32)
            x = xs[t, r, part_span(t, c)].astype(jnp.float32)
            out[t, 0, r, part_span(t, c)] = (x + total).astype(jnp.bfloat16)

        pieces(step)

        @pl.when(hops(t, c))
        def _():
            hop_copy(t, c).start()

    def take(t, c):
        chosen = order[0, t]
        last = t + 1 == ticks

        def step(r, source):
            if source is duo:
                total = duo[1, r, :].astype(jnp.float32)
                for d in range(1, peers):
                    total = total + duo[1 + d, r, :].astype(jnp.float32)
                new = (duo[0, r, :].astype(jnp.float32) + total).astype(jnp.bfloat16)
                new = new.astype(jnp.float32)
            else:
                new = source[t, r, part_span(t, c)].astype(jnp.float32)
            values = [
                jnp.where(chosen == k, new, slots[k, r, part_span(t, c)].astype(jnp.float32))
                for k in range(n_slots)
            ]
            for k in range(n_slots):
                if last:
                    held[0, k, r, part_span(t, c)] = values[k].astype(jnp.bfloat16)
                else:
                    slots[k, r, part_span(t, c)] = values[k].astype(jnp.bfloat16)
            if not last:
                xs[t + 1, r, part_span(t, c)] = pick(t + 1, values).astype(jnp.bfloat16)

        if last and c == both:
            @pl.when(late)
            def _():
                with jax.named_scope("shared_wait"):
                    shared_wait(duo_sem)
                pieces(functools.partial(step, source=duo))

            by_hop = has_prev & early
        else:
            by_hop = has_prev

        @pl.when(by_hop)
        def _():
            with jax.named_scope(f"hop_wait_{t}_{c}"):
                hop_copy(t, c).wait_recv()
            pieces(functools.partial(step, source=arr))

        @pl.when(jnp.logical_not(has_prev))
        def _():
            pieces(functools.partial(step, source=fresh_v))

    def first_rows(i):
        with jax.named_scope(f"acts_wait_{i}"):
            acts_copy(i).wait()
            if i == last_block:
                for n in range(n_tiles):
                    wi_copy(n).start()
                load_wo.start()
                load_fresh.start()
        with jax.named_scope(f"norm_first_{i}"):
            if i:
                norm(0, i)
            else:
                offer(i)

    with jax.named_scope("small_wait"):
        load_order.wait()
        pltpu.make_async_copy(affine, affine, small_sem.at[1]).wait()
    first_rows(0)
    with jax.named_scope("barrier"):
        pl.semaphore_wait(
            barrier,
            (peers - 1) * (1 + leads.astype(jnp.int32))
            + has_prev.astype(jnp.int32) + has_next.astype(jnp.int32),
        )
    for i in range(len(blocks)):
        if i:
            first_rows(i)

        @pl.when(early)
        def _():
            send_rows(0, i)

    norm(0, 0)

    with jax.named_scope("project_first"):
        project(0)

    @pl.when(late)
    def _():
        await_turn(0)
        for i in range(len(blocks)):
            send_rows(0, i)

    yield_turn(0, leads)

    for t in range(ticks):
        if t:
            with jax.named_scope(f"lead_{t}"):
                for d in range(1, peers):
                    sent(t, d, 0)

            yield_turn(3, leads)
            yield_turn(2, late)
            reduced(t - 1)
        for d in range(1, peers):
            if t == 0:
                with jax.named_scope("raw_wait"):
                    raw_copy(d).wait_recv()
                with jax.named_scope("raw_norm"):
                    norm(0, 0, raw.at[d - 1], d)
            for c in range(n_chunks):
                with jax.named_scope(f"ag_wait_{t}_{c}"):
                    ag_copy(t, d, c, slice(None) if t else row_block(last_block)).wait_recv()
                with jax.named_scope(f"pchunk_{t}_{c}"):
                    project_chunk(t, d, c)
        if t == 0:
            load_wo.wait()
        for d in [*range(1, peers), 0]:
            with jax.named_scope(f"attend_{t}_{d}"):
                attend(t, d)
        if t == 0:
            load_fresh.wait()
        if t + 1 == ticks:
            if t:
                hopped(t - 1)

            @pl.when(early)
            def _():
                for c in range(both):
                    finish(t, c)
                for c in range(len(parts[t])):
                    take(t, c)
                finish(t, both)

            @pl.when(late)
            def _():
                for c in range(len(parts[t])):
                    finish(t, c)
                for c in range(len(parts[t])):
                    take(t, c)
        else:
            ahead = max(len(parts[t]) - 3, 0)

            @pl.when(early)
            def _():
                for c in range(len(parts[t])):
                    finish(t, c)
                for c in range(len(parts[t])):
                    take(t, c)

            @pl.when(late)
            def _():
                for c in range(len(parts[t])):
                    take(t, c)
                    if 0 <= c - 2 < ahead:
                        finish(t, c - 2)

            gathered(t)
            for i in range(len(blocks)):
                with jax.named_scope(f"norm_{t}_{i}"):
                    norm(t + 1, i)
                if i == 0:
                    @pl.when(leads)
                    def _():
                        await_turn(2)

                send_rows(t + 1, i)

            @pl.when(late)
            def _():
                for c in range(ahead, len(parts[t])):
                    finish(t, c)

            with jax.named_scope(f"project_{t}"):
                project(t + 1)

    gathered(ticks - 1)
    reduced(ticks - 1)
    hopped(ticks - 1)


def flush(out_v, held_v, out, held, sem):
    copies = [
        pltpu.make_async_copy(out_v, out, sem.at[0]),
        pltpu.make_async_copy(held_v, held, sem.at[1]),
    ]
    for copy in copies:
        copy.start()
    for copy in copies:
        copy.wait()


def pin(*xs):
    return [pltpu.with_memory_space_constraint(x, pltpu.HBM) for x in xs]


def body(acts, fresh, order, ln_gain, ln_bias, wqkv, wo):
    ticks, rows, width = fresh.shape
    n_slots = acts.shape[1]
    peers = lax.axis_size("tensor")
    seq = rows * peers
    n_chunks = len(ag_spans(width))
    n_parts = len(rs_spans(width))
    inner = wo.shape[1]
    wide = wqkv.shape[2]
    bf = jnp.bfloat16
    dma = pltpu.SemaphoreType.DMA
    anywhere = pl.BlockSpec(memory_space=pl.ANY)
    vmem = pl.BlockSpec(memory_space=pltpu.VMEM)
    out_shape = (ticks, 1, rows, width)
    held_shape = (1, n_slots, rows, width)
    results = pl.pallas_call(
        relay,
        out_shape=(pltpu.VMEM(out_shape, bf), pltpu.VMEM(held_shape, bf)),
        in_specs=[anywhere] * 7,
        out_specs=(vmem, vmem),
        scratch_shapes=[
            pltpu.SMEM(order.shape, jnp.int32),
            pltpu.VMEM((2, width), jnp.float32),
            pltpu.VMEM((n_slots, rows, width), bf),
            pltpu.VMEM((ticks, rows, width), bf),
            pltpu.VMEM((width, wide), bf),
            pltpu.VMEM((inner, width), bf),
            pltpu.VMEM((ticks, rows, width), bf),
            pltpu.VMEM((ticks, peers, rows, width), bf),
            pltpu.VMEM((rows, wide), jnp.float32),
            pltpu.VMEM((seq, wide), bf),
            pltpu.VMEM((rows, inner), bf),
            pltpu.VMEM((ticks, peers, rows, width), bf),
            pltpu.VMEM((ticks, peers - 1, rows, width), bf),
            pltpu.VMEM((ticks, rows, width), bf),
            pltpu.VMEM((peers + 1, rows, rs_spans(width)[-1][1]), bf),
            pltpu.VMEM((peers - 1, rows // 8, width), bf),
            dma((2,)),
            dma((2,)),
            dma,
            dma((wide // fitting(TILE, wide),)),
            dma,
            dma((peers - 1, 2)),
            dma((ticks, peers - 1, n_chunks)),
            dma((peers - 1,)),
            dma((ticks, peers - 1, n_parts)),
            dma((ticks, n_parts)),
            dma,
            dma((peers - 1,)),
            pltpu.SemaphoreType.REGULAR((1,)),
        ],
        compiler_params=pltpu.CompilerParams(
            collective_id=0, has_side_effects=True, vmem_limit_bytes=52 * 1024 * 1024
        ),
    )(*pin(acts, fresh, order, ln_gain, ln_bias, wqkv, wo))
    return pl.pallas_call(
        flush,
        out_shape=(jax.ShapeDtypeStruct(out_shape, bf), jax.ShapeDtypeStruct(held_shape, bf)),
        in_specs=[vmem, vmem],
        out_specs=(pl.BlockSpec(memory_space=pltpu.HBM), pl.BlockSpec(memory_space=pltpu.HBM)),
        scratch_shapes=[dma((2,))],
    )(*[pltpu.with_memory_space_constraint(x, pltpu.VMEM) for x in results])


def solution(mesh):
    return jax.shard_map(
        body,
        mesh=mesh,
        in_specs=(
            P("section", "dp", "tensor", None),
            P("dp", "tensor", None),
            P("section", None),
            P("section", None),
            P("section", None),
            P("section", None, "tensor"),
            P("section", "tensor", None),
        ),
        out_specs=(P("dp", "section", "tensor", None), P("section", "dp", "tensor", None)),
        check_vma=False,
    )
```
